128 devices in a mesh: seq: 16 (over z, y), ch: 8 (over x, core).
Axes of the slice: x: 4, y: 4, z: 4, core: 2. Of those that a mesh axis runs over, the one named last changes fastest.
Arguments:
- signal: float32 [1, 65536, 1024], P(None, 'seq', 'ch'), may hold values from -6 to 6
- spectrum: float32 [2, 256, 256, 1024], P(None, 'seq', None, 'ch'), may hold values from -6 to 6
- channel_mode: int32 [1024], P('ch'), may hold values 0 or 1
- skip_gain: float32 [1024], P('ch'), may hold values from -4 to 4
- out_weight: bfloat16 [1024, 1024], P('ch'), may hold values from -0.1875 to 0.1875
Outputs:
- projected: float32 [1, 65536, 1024], P(None, 'seq', 'ch')
The draws below stay inside these ranges and needn't reach their ends.
Inputs may be any that keep to these rules, and one draw needn't show every extreme that they name: `channel_mode`: 1 marks a channel whose 65536 positions are one sequence, 0 a channel whose positions form a 256 x 256 image.
All inputs are finite; a program needn't handle non-finite values. No bound on the sum of `channel_mode` on one device may be relied on, other than what follows from the above.
Results may differ from the reference program's by a relative error of at most 0.017.
Values may be sent and summed in bfloat16 or wider, within the bound.
A program may use at most 128 MiB of HBM per device.

```python
import jax
import jax.numpy as jnp
from jax import lax

BATCH = 1
WIDTH = 1024
ROWS = 256
COLUMNS = 256
LENGTH = 65536
N_CH = 8


def place_ends(values, key, low, high):
    place = [jax.random.randint(jax.random.fold_in(key, axis), (), 0, length) for axis, length in enumerate(values.shape)]
    main_axis = values.shape.index(max(values.shape))
    neighbour = place[:main_axis] + [(place[main_axis] + 1) % values.shape[main_axis]] + place[main_axis + 1:]
    return values.at[tuple(place)].set(low).at[tuple(neighbour)].set(high)


def levels(rng, extent, shards, smallest, largest):
    def one(position, shards_of):
        steps = jax.random.uniform(jax.random.fold_in(jax.random.fold_in(rng, 6), position), (shards_of,), jnp.float32, smallest / len(shards), largest / len(shards))
        return jnp.repeat(jnp.exp(steps), extent[position] // shards_of).reshape((-1,) + (1,) * (len(extent) - position - 1))

    level = one(*shards[0])
    for cut in shards[1:]:
        level = level * one(*cut)
    return level


def centred(stream_key, dims, width, limit, cuts=(), dtype=jnp.bfloat16):
    drawn = width * jax.random.normal(stream_key, dims, jnp.float32)
    if cuts:
        drawn = drawn * levels(stream_key, dims, cuts, -0.22, 0.18)
    return jnp.clip(drawn, -limit, limit).astype(dtype)


def setup_inputs(seed: int = 0) -> dict:
    splits = jax.random.split(jax.random.key(seed), 6)
    signal = centred(splits[0], (BATCH, LENGTH, WIDTH), 1.0, 6.0, ((1, 16), (2, 8)), jnp.float32)
    spectrum = centred(splits[1], (2, ROWS, COLUMNS, WIDTH), 0.7071, 6.0, ((1, 16), (3, 8)), jnp.float32)
    channel_mode = place_ends((jax.random.randint(splits[2], (WIDTH,), 0, 2) < 1).astype(jnp.int32), jax.random.fold_in(splits[2], 1), 0, 1)
    skip_gain = centred(splits[3], (WIDTH,), 1.0, 4.0, ((0, 8),), jnp.float32)
    out_weight = centred(splits[4], (WIDTH, WIDTH), WIDTH ** -0.5, 0.1875, ((0, 8),))
    return {"signal": signal, "spectrum": spectrum, "channel_mode": channel_mode, "skip_gain": skip_gain, "out_weight": out_weight}


def convolve_block(packed):
    signal_block, spectrum_block, mode_block, gain_block = packed
    series = jnp.transpose(signal_block, (0, 2, 1))
    filters = lax.complex(spectrum_block[0], spectrum_block[1])
    filters = jnp.transpose(filters, (2, 0, 1))
    linear_filter = jnp.transpose(filters, (0, 2, 1)).reshape(filters.shape[0], LENGTH)
    linear = jnp.real(jnp.fft.ifft(jnp.fft.fft(series, axis=-1) * linear_filter[None], axis=-1))
    images = series.reshape(series.shape[0], series.shape[1], ROWS, COLUMNS)
    planar = jnp.real(jnp.fft.ifft2(jnp.fft.fft2(images, axes=(-2, -1)) * filters[None], axes=(-2, -1)))
    planar = planar.reshape(series.shape)
    convolved = jnp.where(mode_block[None, :, None] == 1, linear, planar)
    hidden = convolved + gain_block[None, :, None] * series
    return jnp.transpose(hidden, (0, 2, 1)).astype(jnp.float32)


def reference(signal, spectrum, channel_mode, skip_gain, out_weight):
    block_width = WIDTH // N_CH
    signal_parts = jnp.moveaxis(signal.reshape(BATCH, LENGTH, N_CH, block_width), 2, 0)
    spectrum_parts = jnp.moveaxis(spectrum.reshape(2, ROWS, COLUMNS, N_CH, block_width), 3, 0)
    mode_parts = channel_mode.reshape(N_CH, block_width)
    gain_parts = skip_gain.reshape(N_CH, block_width)
    hidden_parts = lax.map(convolve_block, (signal_parts, spectrum_parts, mode_parts, gain_parts))
    hidden_parts = hidden_parts.astype(jnp.bfloat16)
    weight_parts = out_weight.reshape(N_CH, block_width, WIDTH)

    def add_block(running, packed):
        features, weights = packed
        partial_value = jnp.dot(features.reshape(BATCH * LENGTH, block_width), weights, preferred_element_type=jnp.float32)
        partial_value = lax.optimization_barrier(partial_value.astype(jnp.bfloat16))
        return running + partial_value.astype(jnp.float32), jnp.zeros((), jnp.float32)

    initial = jnp.zeros((BATCH * LENGTH, WIDTH), jnp.float32)
    total, unused = lax.scan(add_block, initial, (hidden_parts, weight_parts))
    return total.reshape(BATCH, LENGTH, WIDTH)
```

```python
import math

import jax
import jax.numpy as jnp
import numpy as np
from jax import lax
from jax.experimental import pallas as pl
from jax.experimental.pallas import tpu as pltpu
from jax.sharding import PartitionSpec as P

ROWS = 256
COLUMNS = 256
LENGTH = 65536
BF16 = jnp.bfloat16
F32 = jnp.float32
MESH = pl.DeviceIdType.MESH


def tables():
    counter = np.arange(256)
    angle = (counter[:, None] * counter[None, :] % 256) * (2.0 * math.pi / 256)
    c, s = np.cos(angle), np.sin(angle)
    first = np.concatenate([c, -s], 0)
    second = np.block([[c, -s], [s, c]])
    third = np.block([[c, s], [-s, c]])
    last = np.concatenate([c, -s], 1) / LENGTH
    twist = counter[:, None] * counter[None, :] * (2.0 * math.pi / LENGTH)
    twist = np.stack([np.cos(twist), np.sin(twist)])
    scatter = np.zeros((64, 64))
    for m in range(4):
        for a in range(16):
            x, k, a2 = a // 4, a // 2 % 2, a % 2
            scatter[((k * 4 + x) * 2 + a2) * 4 + m, m * 16 + a] = 1
    regroup = np.zeros((256, 256))
    for h in range(2):
        for s in range(16):
            for a2 in range(2):
                for m in range(4):
                    regroup[((h * 16 + s) * 2 + a2) * 4 + m, a2 * 128 + s * 8 + h * 4 + m] = 1
    half = [jnp.asarray(t, BF16) for t in (first, second, third, last, scatter, regroup)]
    return half + [jnp.asarray(twist, F32)]


def flip(v, mask):
    if mask == 0:
        return v
    if mask == 1:
        return v + 1 - 2 * lax.rem(v, 2)
    if mask == 2:
        return lax.rem(v + 2, 4)
    return 3 - v


def dot(a, b):
    return jnp.dot(a, b, preferred_element_type=F32)


def kernel(
    src, w, mode, gain, first, second, third, last, scatter, regroup, twist,
    out,
    zrel, zbuf, yrel, final, spectral, hid, send, bzrel, bzbuf, byrel, bfinal,
    swap, xrel, gathered, rows, wfull, prod, swap2, xrel2,
    a_sems, b_sems, w_sems, c_sems, d_sems,
):
    s = lax.axis_index("seq")
    c = lax.axis_index("ch")
    z, y, x, k = s // 4, lax.rem(s, 4), c // 2, lax.rem(c, 2)
    other = 1 - k

    def zdev(mask):
        return {"seq": flip(z, mask) * 4 + y, "ch": c}

    def ydev(mask):
        return {"seq": z * 4 + flip(y, mask), "ch": c}

    def xdev(mask):
        return {"seq": s, "ch": flip(x, mask) * 2 + k}

    partner = {"seq": s, "ch": x * 2 + other}

    def copy(a, b, ss, rs, dev):
        return pltpu.make_async_remote_copy(a, b, ss, rs, device_id=dev, device_id_type=MESH)

    def recv(ref, sem):
        copy(ref, ref, sem, sem, partner).wait_recv()

    def sent(ref, sem):
        copy(ref, ref, sem, sem, partner).wait_send()

    barrier = pltpu.get_barrier_semaphore()
    for dev in (zdev(1), zdev(3), ydev(1), ydev(3), xdev(1), xdev(3), partner):
        pl.semaphore_signal(barrier, 1, device_id=dev, device_id_type=MESH)
    pl.semaphore_wait(barrier, 7)

    class Plane:
        def __init__(self, src, zrel, zbuf, yrel, final, sems):
            self.src, self.zrel, self.zbuf, self.yrel, self.final = src, zrel, zbuf, yrel, final
            self.sz, self.sy, self.rzrel, self.rfin, self.rz, self.ryrel = sems

        def zsend(self, q):
            def part(mask):
                return self.src.at[q, pl.ds(4 * flip(z, mask), 4)]

            copy(part(2), self.zrel.at[q], self.sz.at[q], self.rzrel.at[q], zdev(1)).start()
            copy(part(3), self.zbuf.at[q, 2], self.sz.at[q], self.rz.at[q, 2], zdev(3)).start()
            copy(part(1), self.zbuf.at[q, 0], self.sz.at[q], self.rz.at[q, 0], zdev(1)).start()

        def zfwd(self, q):
            recv(self.zrel.at[q], self.rzrel.at[q])
            copy(
                self.zrel.at[q], self.zbuf.at[q, 1], self.sz.at[q], self.rz.at[q, 1], zdev(3)
            ).start()

        def ysend(self, q, mz):
            if mz:
                recv(self.zbuf.at[q, mz - 1], self.rz.at[q, mz - 1])

            def part(mask):
                if mz:
                    return self.zbuf.at[q, mz - 1, flip(y, mask)]
                return self.src.at[q, z * 4 + flip(y, mask)]

            slot = self.final.at[q, flip(z, mz) * 4 + y]
            copy(part(2), self.yrel.at[q, mz], self.sy.at[q], self.ryrel.at[q, mz], ydev(1)).start()
            copy(part(3), slot, self.sy.at[q], self.rfin.at[q], ydev(3)).start()
            copy(part(1), slot, self.sy.at[q], self.rfin.at[q], ydev(1)).start()
            slot[...] = part(0)[...]

        def yfwd(self, q, mz):
            recv(self.yrel.at[q, mz], self.ryrel.at[q, mz])
            slot = self.final.at[q, flip(z, mz) * 4 + flip(y, 1)]
            copy(self.yrel.at[q, mz], slot, self.sy.at[q], self.rfin.at[q], ydev(3)).start()

        def done(self, q):
            recv(self.final.at[q, pl.ds(0, 12)], self.rfin.at[q])

        def drain(self, q):
            sent(self.src.at[q], self.sz.at[q])
            sent(self.src.at[q], self.sy.at[q])

    first_plane = Plane(src, zrel, zbuf, yrel, final, a_sems)
    back = Plane(send, bzrel, bzbuf, byrel, bfinal, b_sems)
    A = first_plane

    def forward(h):
        def step(m, carry):
            image = final[0, :, h, m].reshape(256, 256)
            value = dot(first[...], image)
            re, im = value[:256], value[256:]
            on = mode[4 * h + m] > 0.5
            tc, ts = jnp.where(on, twist[0], 1.0), jnp.where(on, twist[1], 0.0)
            pair = jnp.concatenate([re * tc + im * ts, im * tc - re * ts], 1).astype(BF16)
            spectral[4 * h + m] = dot(pair, second[...])
            return carry

        lax.fori_loop(0, 4, step, 0)

    def inverse(h):
        def step(m, carry):
            value = spectral[4 * h + m]
            re, im = value[:, :256], value[:, 256:]
            fr = final[1 + h, :, 0, m].reshape(256, 256).astype(F32)
            fi = final[1 + h, :, 1, m].reshape(256, 256).astype(F32)
            pair = jnp.concatenate([re * fr - im * fi, re * fi + im * fr], 1).astype(BF16)
            value = dot(pair, third[...])
            re, im = value[:, :256], value[:, 256:]
            on = mode[4 * h + m] > 0.5
            tc, ts = jnp.where(on, twist[0], 1.0), jnp.where(on, twist[1], 0.0)
            pair = jnp.concatenate([re * tc - im * ts, re * ts + im * tc], 0).astype(BF16)
            value = dot(last[...], pair)
            image = final[0, :, h, m].reshape(256, 256).astype(F32)
            value = value + gain[4 * h + m] * image
            hid[m] = value.astype(BF16).reshape(16, 16, 256)
            return carry

        lax.fori_loop(0, 4, step, 0)

        def place(t, carry):
            block = hid[:, t].reshape(64, 256)
            send[h, t] = dot(scatter[...], block).astype(BF16).reshape(2, 4, 8, 256)
            return carry

        lax.fori_loop(0, 16, place, 0)

    A.zsend(0)
    A.ysend(0, 0)
    A.zsend(1)
    A.ysend(1, 0)
    A.ysend(2, 0)

    own = pl.ds(pl.multiple_of(c * 128, 128), 128)

    def wrows(mask):
        return wfull.at[pl.ds(pl.multiple_of((flip(x, mask) * 2 + k) * 128, 128), 128)]

    ws, wx, wp = w_sems
    copy(w, wfull.at[own], ws, wx.at[0], xdev(1)).start()
    copy(w, wfull.at[own], ws, wx.at[2], xdev(3)).start()
    copy(w, wfull.at[own], ws, wp.at[0], partner).start()
    wfull[own] = w[...]

    A.yfwd(0, 0)
    A.zfwd(0)
    A.zsend(2)
    A.ysend(0, 3)
    A.yfwd(1, 0)
    A.yfwd(2, 0)
    recv(wrows(1), wx.at[0])
    copy(wrows(1), wrows(1), ws, wx.at[1], xdev(3)).start()
    copy(wrows(1), wrows(1), ws, wp.at[1], partner).start()
    A.ysend(0, 1)
    A.ysend(1, 3)
    A.yfwd(0, 3)
    A.yfwd(0, 1)
    A.zfwd(1)
    recv(wrows(3), wx.at[2])
    copy(wrows(3), wrows(3), ws, wp.at[3], partner).start()
    A.ysend(0, 2)
    A.yfwd(1, 3)
    A.ysend(1, 1)
    A.yfwd(0, 2)
    recv(wrows(2), wx.at[1])
    copy(wrows(2), wrows(2), ws, wp.at[2], partner).start()
    A.ysend(2, 3)
    A.zfwd(2)
    A.yfwd(1, 1)
    A.done(0)
    forward(0)
    A.ysend(1, 2)
    A.yfwd(2, 3)
    A.yfwd(1, 2)
    forward(1)
    A.ysend(2, 1)
    A.ysend(2, 2)
    A.done(1)
    inverse(0)
    back.zsend(0)
    A.yfwd(2, 1)
    A.yfwd(2, 2)
    back.ysend(0, 0)
    back.yfwd(0, 0)
    back.zfwd(0)
    A.done(2)
    inverse(1)
    back.zsend(1)
    back.ysend(0, 3)
    back.ysend(0, 1)
    back.ysend(1, 0)
    back.yfwd(0, 3)
    back.yfwd(0, 1)
    back.ysend(0, 2)
    back.zfwd(1)
    back.yfwd(1, 0)
    back.yfwd(0, 2)

    es, er, xs, xr, fr = c_sems

    def xsend(h, i):
        kept = k if i == 0 else other

        def part(mask):
            if i == 0:
                return bfinal.at[h, :, k, flip(x, mask)]
            return swap.at[h, :, flip(x, mask)]

        slot = gathered.at[x, kept, h]
        copy(part(2), xrel.at[h, i], xs, xr.at[h, i], xdev(1)).start()
        copy(part(3), slot, xs, fr, xdev(3)).start()
        copy(part(1), slot, xs, fr, xdev(1)).start()
        slot[...] = part(0)[...]

    def xfwd(h, i):
        kept = k if i == 0 else other
        recv(xrel.at[h, i], xr.at[h, i])
        copy(xrel.at[h, i], gathered.at[flip(x, 1), kept, h], xs, fr, xdev(3)).start()

    def exchange(h):
        back.done(h)
        copy(bfinal.at[h, :, other], swap.at[h], es, er.at[h], partner).start()
        xsend(h, 0)

    exchange(0)
    back.ysend(1, 3)
    back.ysend(1, 1)
    recv(swap.at[0], er.at[0])
    xsend(0, 1)
    back.yfwd(1, 3)
    back.yfwd(1, 1)
    back.ysend(1, 2)
    xfwd(0, 0)
    back.yfwd(1, 2)
    xfwd(0, 1)
    exchange(1)
    recv(swap.at[1], er.at[1])
    xsend(1, 1)
    xfwd(1, 0)
    xfwd(1, 1)
    for mask in range(4):
        recv(wfull.at[pl.ds(0, 128)], wp.at[mask])
    recv(gathered.at[pl.ds(0, 3)], fr)

    for i in range(8):
        block = gathered[i // 2, i % 2].reshape(256, 256)
        value = lax.dot_general(
            block, regroup[...], (((0,), (0,)), ((), ())), preferred_element_type=F32
        ).astype(BF16)
        rows[0, :, i * 128 : (i + 1) * 128] = value[:, :128]
        rows[1, :, i * 128 : (i + 1) * 128] = value[:, 128:]

    for i in range(4):
        value = dot(rows[...].reshape(512, 1024), wfull[:, i * 256 : (i + 1) * 256]).astype(BF16)
        prod[0, i] = value[:, :128]
        prod[1, i] = value[:, 128:]

    ds, dr, dxs, dxr, dout = d_sems
    copy(prod.at[other], swap2, ds, dr, partner).start()

    def osend(i):
        kept = k if i == 0 else other

        def part(mask):
            if i == 0:
                return prod.at[k, flip(x, mask)]
            return swap2.at[flip(x, mask)]

        slot = out.at[x * 2 + kept]
        copy(part(2), xrel2.at[i], dxs, dxr.at[i], xdev(1)).start()
        copy(part(3), slot, dxs, dout, xdev(3)).start()
        copy(part(1), slot, dxs, dout, xdev(1)).start()
        slot[...] = part(0)[...]

    def ofwd(i):
        kept = k if i == 0 else other
        recv(xrel2.at[i], dxr.at[i])
        copy(xrel2.at[i], out.at[flip(x, 1) * 2 + kept], dxs, dout, xdev(3)).start()

    osend(0)
    recv(swap2, dr)
    osend(1)
    ofwd(0)
    ofwd(1)
    recv(out.at[pl.ds(0, 6)], dout)

    for q in range(3):
        A.drain(q)
    for h in range(2):
        back.drain(h)
    sent(wfull.at[pl.ds(0, 7 * 128)], ws)
    sent(swap, es)
    sent(gathered, xs)
    sent(swap2, ds)
    sent(out, dxs)


def per_device(signal, spectrum, channel_mode, skip_gain, out_weight):
    s = lax.axis_index("seq")
    pieces = signal.reshape(16, 256, 128).astype(BF16).transpose(2, 0, 1)
    pieces = pieces.reshape(1, 16, 2, 4, 16, 256)
    filters = spectrum.astype(BF16).reshape(2, 16, 256, 16, 2, 4)
    filters = filters.transpose(4, 3, 0, 5, 1, 2)
    source = jnp.concatenate([pieces, filters], 0)
    mode = lax.dynamic_slice_in_dim(channel_mode, s * 8, 8).astype(F32)
    gain = lax.dynamic_slice_in_dim(skip_gain, s * 8, 8)
    unit = (2, 4, 16, 256)
    small = (2, 4, 8, 256)
    dma = pltpu.SemaphoreType.DMA

    def plane(n):
        return (dma((n,)), dma((n,)), dma((n,)), dma((n,)), dma((n, 3)), dma((n, 4)))

    vmem = pl.BlockSpec(memory_space=pltpu.VMEM)
    smem = pl.BlockSpec(memory_space=pltpu.SMEM)
    result = pl.pallas_call(
        kernel,
        out_shape=jax.ShapeDtypeStruct((8, 512, 128), BF16),
        in_specs=[vmem, vmem, smem, smem] + [vmem] * 7,
        out_specs=vmem,
        scratch_shapes=[
            pltpu.VMEM((3, 4) + unit, BF16),
            pltpu.VMEM((3, 3, 4) + unit, BF16),
            pltpu.VMEM((3, 4) + unit, BF16),
            pltpu.VMEM((3, 16) + unit, BF16),
            pltpu.VMEM((8, 256, 512), F32),
            pltpu.VMEM((4, 16, 16, 256), BF16),
            pltpu.VMEM((2, 16) + small, BF16),
            pltpu.VMEM((2, 4) + small, BF16),
            pltpu.VMEM((2, 3, 4) + small, BF16),
            pltpu.VMEM((2, 4) + small, BF16),
            pltpu.VMEM((2, 16) + small, BF16),
            pltpu.VMEM((2, 16, 4, 8, 256), BF16),
            pltpu.VMEM((2, 2, 16, 8, 256), BF16),
            pltpu.VMEM((4, 2, 2, 16, 8, 256), BF16),
            pltpu.VMEM((2, 256, 1024), BF16),
            pltpu.VMEM((1024, 1024), BF16),
            pltpu.VMEM((2, 4, 512, 128), BF16),
            pltpu.VMEM((4, 512, 128), BF16),
            pltpu.VMEM((2, 512, 128), BF16),
            plane(3),
            plane(2),
            (dma, dma((3,)), dma((4,))),
            (dma, dma((2,)), dma, dma((2, 2)), dma),
            (dma, dma, dma, dma((2,)), dma),
        ],
        compiler_params=pltpu.CompilerParams(
            collective_id=0, has_side_effects=True, vmem_limit_bytes=60 << 20
        ),
        name="hyena",
    )(source, out_weight, mode, gain, *tables())
    return result.astype(F32).reshape(1, 4096, 128)


def solution(mesh):
    in_specs = (
        P(None, "seq", "ch"), P(None, "seq", None, "ch"), P("ch"), P("ch"), P("ch", None)
    )
    return jax.shard_map(
        per_device, mesh=mesh, in_specs=in_specs, out_specs=P(None, "seq", "ch"), check_vma=False
    )
```

```python
import math

import jax
import jax.numpy as jnp
import numpy as np
from jax import lax
from jax.experimental import pallas as pl
from jax.experimental.pallas import tpu as pltpu
from jax.sharding import PartitionSpec as P

ROWS = 256
COLUMNS = 256
LENGTH = 65536
BF16 = jnp.bfloat16
F32 = jnp.float32
MESH = pl.DeviceIdType.MESH


def tables():
    counter = np.arange(256)
    angle = (counter[:, None] * counter[None, :] % 256) * (2.0 * math.pi / 256)
    c, s = np.cos(angle), np.sin(angle)
    first = np.concatenate([c, -s], 0)
    second = np.block([[c, -s], [s, c]])
    third = np.block([[c, s], [-s, c]])
    last = np.concatenate([c, -s], 1) / LENGTH
    twist = counter[:, None] * counter[None, :] * (2.0 * math.pi / LENGTH)
    twist = np.stack([np.cos(twist), np.sin(twist)])
    scatter = np.zeros((256, 256))
    for m in range(4):
        for t in range(4):
            for a in range(16):
                x, k, a2 = a // 4, a // 2 % 2, a % 2
                scatter[t * 64 + ((k * 4 + x) * 2 + a2) * 4 + m, (m * 4 + t) * 16 + a] = 1
    regroup = np.zeros((256, 256))
    for h in range(2):
        for s in range(16):
            for a2 in range(2):
                for m in range(4):
                    regroup[((h * 16 + s) * 2 + a2) * 4 + m, a2 * 128 + s * 8 + h * 4 + m] = 1
    half = [jnp.asarray(t, BF16) for t in (first, second, third, last, scatter, regroup)]
    return half + [jnp.asarray(twist, F32)]


def flip(v, mask):
    if mask == 0:
        return v
    if mask == 1:
        return v + 1 - 2 * lax.rem(v, 2)
    if mask == 2:
        return lax.rem(v + 2, 4)
    return 3 - v


def dot(a, b):
    return jnp.dot(a, b, preferred_element_type=F32)


def kernel(
    sig, spec, w, mode, gain, first, second, third, last, scatter, regroup, twist,
    out,
    rel1, buf, rel2, final, spectral, hid, send, brel1, bbuf, brel2, bfinal,
    swap, xrel, gathered, rows, wfull, prod, swap2, xrel2,
    a_sems, b_sems, w_sems, c_sems, d_sems,
):
    s = lax.axis_index("seq")
    c = lax.axis_index("ch")
    z, y, x, k = s // 4, lax.rem(s, 4), c // 2, lax.rem(c, 2)
    other = 1 - k

    def zdev(mask):
        return {"seq": flip(z, mask) * 4 + y, "ch": c}

    def ydev(mask):
        return {"seq": z * 4 + flip(y, mask), "ch": c}

    def xdev(mask):
        return {"seq": s, "ch": flip(x, mask) * 2 + k}

    partner = {"seq": s, "ch": x * 2 + other}

    def copy(a, b, ss, rs, dev):
        return pltpu.make_async_remote_copy(a, b, ss, rs, device_id=dev, device_id_type=MESH)

    def recv(ref, sem):
        copy(ref, ref, sem, sem, partner).wait_recv()

    def sent(ref, sem):
        copy(ref, ref, sem, sem, partner).wait_send()

    barrier = pltpu.get_barrier_semaphore()
    for dev in (zdev(1), zdev(3), ydev(1), ydev(3), xdev(1), xdev(3), partner):
        pl.semaphore_signal(barrier, 1, device_id=dev, device_id_type=MESH)
    pl.semaphore_wait(barrier, 7)

    class Plane:
        def __init__(self, grab, rel1, buf, rel2, final, sems):
            self.grab, self.rel1, self.buf, self.rel2, self.final = grab, rel1, buf, rel2, final
            self.s1, self.s2, self.rrel1, self.rfin, self.rbuf, self.rrel2 = sems

        def dev(self, u, leg, mask):
            return zdev(mask) if u % 2 == leg else ydev(mask)

        def slot(self, u, m1, m2):
            if u % 2 == 0:
                return self.final.at[u, flip(z, m1), flip(y, m2)]
            return self.final.at[u, flip(z, m2), flip(y, m1)]

        def row(self, u, mask):
            if u % 2 == 0:
                return self.grab(u, flip(z, mask), slice(None))
            return self.grab(u, slice(None), flip(y, mask))

        def F(self, u):
            one, three = self.dev(u, 0, 1), self.dev(u, 0, 3)
            s1, rb = self.s1.at[u], self.rbuf
            copy(self.row(u, 2), self.rel1.at[u], s1, self.rrel1.at[u], one).start()
            copy(self.row(u, 3), self.buf.at[u, 2], s1, rb.at[u, 2], three).start()
            copy(self.row(u, 1), self.buf.at[u, 0], s1, rb.at[u, 0], one).start()

        def R(self, u):
            recv(self.rel1.at[u], self.rrel1.at[u])
            three = self.dev(u, 0, 3)
            copy(
                self.rel1.at[u], self.buf.at[u, 1], self.s1.at[u], self.rbuf.at[u, 1], three
            ).start()

        def S(self, u, m1):
            if m1:
                recv(self.buf.at[u, m1 - 1], self.rbuf.at[u, m1 - 1])

            def part(mask):
                other = flip(y if u % 2 == 0 else z, mask)
                if m1:
                    return self.buf.at[u, m1 - 1, other]
                return self.grab(u, z, other) if u % 2 == 0 else self.grab(u, other, y)

            slot = self.slot(u, m1, 0)
            one, three = self.dev(u, 1, 1), self.dev(u, 1, 3)
            s2, done = self.s2.at[u], self.rfin.at[u]
            copy(part(2), self.rel2.at[u, m1], s2, self.rrel2.at[u, m1], one).start()
            copy(part(3), slot, s2, done, three).start()
            copy(part(1), slot, s2, done, one).start()
            slot[...] = part(0)[...]

        def T(self, u, m1):
            recv(self.rel2.at[u, m1], self.rrel2.at[u, m1])
            slot = self.slot(u, m1, 1)
            three = self.dev(u, 1, 3)
            copy(self.rel2.at[u, m1], slot, self.s2.at[u], self.rfin.at[u], three).start()

        def done(self, u):
            recv(self.final.at[u, pl.ds(0, 3)], self.rfin.at[u])

        def drain(self, u):
            sent(self.final.at[u], self.s1.at[u])
            sent(self.final.at[u], self.s2.at[u])

    def grab_inputs(u, zi, yi):
        if u < 2:
            return sig.at[zi, yi, u]
        return spec.at[u % 2, zi, yi, u // 2 - 1]

    A = Plane(grab_inputs, rel1, buf, rel2, final, a_sems)
    B = Plane(lambda u, zi, yi: send.at[u, zi, yi], brel1, bbuf, brel2, bfinal, b_sems)

    def twists(ch):
        on = mode[s * 8 + ch] == 1
        return jnp.where(on, twist[0], 1.0), jnp.where(on, twist[1], 0.0)

    def forward(h, lo):
        def step(m, carry):
            image = final[h, :, :, m].reshape(256, 256)
            value = dot(first[...], image)
            re, im = value[:256], value[256:]
            tc, ts = twists(4 * h + m)
            pair = jnp.concatenate([re * tc + im * ts, im * tc - re * ts], 1).astype(BF16)
            spectral[4 * h + m] = dot(pair, second[...])
            return carry

        lax.fori_loop(lo, lo + 2, step, 0)

    def inverse(h, lo):
        def step(m, carry):
            value = spectral[4 * h + m]
            re, im = value[:, :256], value[:, 256:]
            fr = final[2 + 2 * h, :, :, m].reshape(256, 256).astype(F32)
            fi = final[3 + 2 * h, :, :, m].reshape(256, 256).astype(F32)
            pair = jnp.concatenate([re * fr - im * fi, re * fi + im * fr], 1).astype(BF16)
            value = dot(pair, third[...])
            re, im = value[:, :256], value[:, 256:]
            tc, ts = twists(4 * h + m)
            pair = jnp.concatenate([re * tc - im * ts, re * ts + im * tc], 0).astype(BF16)
            value = dot(last[...], pair)
            image = final[h, :, :, m].reshape(256, 256).astype(F32)
            value = value + gain[s * 8 + 4 * h + m] * image
            hid[m] = value.astype(BF16).reshape(4, 4, 16, 256)
            return carry

        lax.fori_loop(lo, lo + 2, step, 0)

    def place(h):
        for t in range(4):
            block = hid[:, t].reshape(256, 256)
            send[h, t] = dot(scatter[...], block).astype(BF16).reshape(4, 2, 4, 8, 256)

    own = pl.ds(pl.multiple_of(c * 128, 128), 128)

    def wrows(mask):
        return wfull.at[pl.ds(pl.multiple_of((flip(x, mask) * 2 + k) * 128, 128), 128)]

    ws, wx, wp = w_sems

    def pair(method, u, *m):
        method(u, *m)
        method(u + 1, *m)

    pair(A.F, 0)
    pair(A.S, 0, 0)
    pair(A.F, 2)
    copy(w, wfull.at[own], ws, wx.at[0], xdev(1)).start()
    copy(w, wfull.at[own], ws, wx.at[2], xdev(3)).start()
    copy(w, wfull.at[own], ws, wp.at[0], partner).start()
    wfull[own] = w[...]
    pair(A.R, 0)
    pair(A.F, 4)
    pair(A.S, 0, 3)
    pair(A.T, 0, 0)
    pair(A.S, 2, 0)
    pair(A.S, 0, 1)
    pair(A.T, 0, 3)
    pair(A.R, 2)
    pair(A.S, 0, 2)
    pair(A.T, 0, 1)
    recv(wrows(1), wx.at[0])
    copy(wrows(1), wrows(1), ws, wx.at[1], xdev(3)).start()
    copy(wrows(1), wrows(1), ws, wp.at[1], partner).start()
    pair(A.S, 2, 3)
    pair(A.T, 2, 0)
    pair(A.S, 4, 0)
    pair(A.T, 0, 2)
    recv(wrows(3), wx.at[2])
    copy(wrows(3), wrows(3), ws, wp.at[3], partner).start()
    pair(A.R, 4)
    pair(A.S, 2, 1)
    pair(A.T, 2, 3)
    A.done(0)
    forward(0, 0)
    pair(A.S, 2, 2)
    pair(A.T, 2, 1)
    recv(wrows(2), wx.at[1])
    copy(wrows(2), wrows(2), ws, wp.at[2], partner).start()
    pair(A.S, 4, 3)
    forward(0, 2)
    pair(A.T, 4, 0)
    pair(A.T, 2, 2)
    A.done(1)
    forward(1, 0)
    pair(A.S, 4, 1)
    pair(A.T, 4, 3)
    forward(1, 2)
    pair(A.S, 4, 2)
    A.done(2)
    A.done(3)
    inverse(0, 0)
    pair(A.T, 4, 1)
    inverse(0, 2)
    pair(A.T, 4, 2)
    place(0)
    B.F(0)
    B.S(0, 0)
    A.done(4)
    A.done(5)
    inverse(1, 0)
    B.R(0)
    B.S(0, 3)
    B.T(0, 0)
    inverse(1, 2)
    place(1)
    B.F(1)
    B.S(1, 0)
    B.S(0, 1)
    B.T(0, 3)
    B.S(0, 2)
    B.R(1)
    B.T(0, 1)
    B.S(1, 3)
    B.T(1, 0)
    B.T(0, 2)

    es, er, xs, xr, fr = c_sems

    def xsend(h, i):
        kept = k if i == 0 else other

        def part(mask):
            if i == 0:
                return bfinal.at[h, :, :, k, flip(x, mask)]
            return swap.at[h, :, :, flip(x, mask)]

        slot = gathered.at[x, kept, h]
        copy(part(2), xrel.at[h, i], xs, xr.at[h, i], xdev(1)).start()
        copy(part(3), slot, xs, fr, xdev(3)).start()
        copy(part(1), slot, xs, fr, xdev(1)).start()
        slot[...] = part(0)[...]

    def xfwd(h, i):
        kept = k if i == 0 else other
        recv(xrel.at[h, i], xr.at[h, i])
        copy(xrel.at[h, i], gathered.at[flip(x, 1), kept, h], xs, fr, xdev(3)).start()

    def exchange(h):
        B.done(h)
        copy(bfinal.at[h, :, :, other], swap.at[h], es, er.at[h], partner).start()
        xsend(h, 0)

    exchange(0)
    B.S(1, 1)
    B.T(1, 3)
    recv(swap.at[0], er.at[0])
    xsend(0, 1)
    B.S(1, 2)
    B.T(1, 1)
    xfwd(0, 0)
    B.T(1, 2)
    xfwd(0, 1)
    exchange(1)
    recv(swap.at[1], er.at[1])
    xsend(1, 1)
    xfwd(1, 0)
    xfwd(1, 1)
    for mask in range(4):
        recv(wfull.at[pl.ds(0, 128)], wp.at[mask])
    recv(gathered.at[pl.ds(0, 3)], fr)

    for i in range(8):
        block = gathered[i // 2, i % 2].reshape(256, 256)
        value = lax.dot_general(
            block, regroup[...], (((0,), (0,)), ((), ())), preferred_element_type=F32
        ).astype(BF16)
        rows[0, :, i * 128 : (i + 1) * 128] = value[:, :128]
        rows[1, :, i * 128 : (i + 1) * 128] = value[:, 128:]

    for i in range(4):
        value = dot(rows[...].reshape(512, 1024), wfull[:, i * 256 : (i + 1) * 256]).astype(BF16)
        prod[0, i] = value[:, :128]
        prod[1, i] = value[:, 128:]

    ds, dr, dxs, dxr, dout = d_sems
    copy(prod.at[other], swap2, ds, dr, partner).start()

    def osend(i):
        kept = k if i == 0 else other

        def part(mask):
            if i == 0:
                return prod.at[k, flip(x, mask)]
            return swap2.at[flip(x, mask)]

        slot = out.at[x * 2 + kept]
        copy(part(2), xrel2.at[i], dxs, dxr.at[i], xdev(1)).start()
        copy(part(3), slot, dxs, dout, xdev(3)).start()
        copy(part(1), slot, dxs, dout, xdev(1)).start()
        slot[...] = part(0)[...]

    def ofwd(i):
        kept = k if i == 0 else other
        recv(xrel2.at[i], dxr.at[i])
        copy(xrel2.at[i], out.at[flip(x, 1) * 2 + kept], dxs, dout, xdev(3)).start()

    osend(0)
    recv(swap2, dr)
    osend(1)
    ofwd(0)
    ofwd(1)
    recv(out.at[pl.ds(0, 6)], dout)

    for u in range(6):
        A.drain(u)
    for h in range(2):
        B.drain(h)
    sent(wfull.at[pl.ds(0, 7 * 128)], ws)
    sent(swap, es)
    sent(gathered, xs)
    sent(swap2, ds)
    sent(out, dxs)


def per_device(signal, spectrum, channel_mode, skip_gain, out_weight):
    pieces = signal.reshape(16, 256, 128).astype(BF16).transpose(2, 0, 1)
    pieces = pieces.reshape(4, 4, 2, 4, 16, 256)
    filters = spectrum.astype(BF16).transpose(0, 3, 1, 2)
    filters = filters.reshape(2, 4, 4, 2, 4, 16, 256)
    unit = (4, 16, 256)
    small = (2, 4, 8, 256)
    dma = pltpu.SemaphoreType.DMA

    def plane(n):
        return (dma((n,)), dma((n,)), dma((n,)), dma((n,)), dma((n, 3)), dma((n, 4)))

    vmem = pl.BlockSpec(memory_space=pltpu.VMEM)
    smem = pl.BlockSpec(memory_space=pltpu.SMEM)
    result = pl.pallas_call(
        kernel,
        out_shape=jax.ShapeDtypeStruct((8, 512, 128), BF16),
        in_specs=[vmem, vmem, vmem, smem, smem] + [vmem] * 7,
        out_specs=vmem,
        scratch_shapes=[
            pltpu.VMEM((6, 4) + unit, BF16),
            pltpu.VMEM((6, 3, 4) + unit, BF16),
            pltpu.VMEM((6, 4) + unit, BF16),
            pltpu.VMEM((6, 4, 4) + unit, BF16),
            pltpu.VMEM((8, 256, 512), F32),
            pltpu.VMEM((4, 4, 4, 16, 256), BF16),
            pltpu.VMEM((2, 4, 4) + small, BF16),
            pltpu.VMEM((2, 4) + small, BF16),
            pltpu.VMEM((2, 3, 4) + small, BF16),
            pltpu.VMEM((2, 4) + small, BF16),
            pltpu.VMEM((2, 4, 4) + small, BF16),
            pltpu.VMEM((2, 4, 4, 4, 8, 256), BF16),
            pltpu.VMEM((2, 2, 4, 4, 8, 256), BF16),
            pltpu.VMEM((4, 2, 2, 4, 4, 8, 256), BF16),
            pltpu.VMEM((2, 256, 1024), BF16),
            pltpu.VMEM((1024, 1024), BF16),
            pltpu.VMEM((2, 4, 512, 128), BF16),
            pltpu.VMEM((4, 512, 128), BF16),
            pltpu.VMEM((2, 512, 128), BF16),
            plane(6),
            plane(2),
            (dma, dma((3,)), dma((4,))),
            (dma, dma((2,)), dma, dma((2, 2)), dma),
            (dma, dma, dma, dma((2,)), dma),
        ],
        compiler_params=pltpu.CompilerParams(
            collective_id=0, has_side_effects=True, vmem_limit_bytes=40 << 20
        ),
        name="hyena",
    )(pieces, filters, out_weight, channel_mode, skip_gain, *tables())
    return result.astype(F32).reshape(1, 4096, 128)


def solution(mesh):
    in_specs = (
        P(None, "seq", "ch"), P(None, "seq", None, "ch"), P("ch"), P("ch"), P("ch", None)
    )
    return jax.shard_map(
        per_device, mesh=mesh, in_specs=in_specs, out_specs=P(None, "seq", "ch"), check_vma=False
    )
```

```python
import math

import jax
import jax.numpy as jnp
import numpy as np
from jax import lax
from jax.experimental import pallas as pl
from jax.experimental.pallas import tpu as pltpu
from jax.sharding import PartitionSpec as P

ROWS = 256
COLUMNS = 256
LENGTH = 65536
BF16 = jnp.bfloat16
F32 = jnp.float32
MESH = pl.DeviceIdType.MESH


def tables():
    counter = np.arange(256)
    angle = (counter[:, None] * counter[None, :] % 256) * (2.0 * math.pi / 256)
    c, s = np.cos(angle), np.sin(angle)
    first = np.concatenate([c, -s], 0)
    second = np.block([[c, -s], [s, c]])
    third = np.block([[c, s], [-s, c]])
    last = np.concatenate([c, -s], 1) / LENGTH
    twist = counter[:, None] * counter[None, :] * (2.0 * math.pi / LENGTH)
    twist = np.stack([np.cos(twist), np.sin(twist)])
    scatter = np.zeros((256, 256))
    for m in range(4):
        for t in range(4):
            for a in range(16):
                x, k, a2 = a // 4, a // 2 % 2, a % 2
                scatter[t * 64 + ((k * 4 + x) * 2 + a2) * 4 + m, (m * 4 + t) * 16 + a] = 1
    regroup = np.zeros((256, 256))
    for h in range(2):
        for s in range(16):
            for a2 in range(2):
                for m in range(4):
                    regroup[((h * 16 + s) * 2 + a2) * 4 + m, a2 * 128 + s * 8 + h * 4 + m] = 1
    half = [jnp.asarray(t, BF16) for t in (first, second, third, last, scatter, regroup)]
    return half + [jnp.asarray(twist, F32)]


def flip(v, mask):
    if mask == 0:
        return v
    if mask == 1:
        return v + 1 - 2 * lax.rem(v, 2)
    if mask == 2:
        return lax.rem(v + 2, 4)
    return 3 - v


def dot(a, b):
    return jnp.dot(a, b, preferred_element_type=F32)


def kernel(
    sig, spec, w, mode, gain, *refs
):
    tables_hbm, (
        out, first, second, third, last, scatter, regroup, twist,
        buf, final, spectral, hid, send, gathered, rows, wfull, prod,
        t_sems, a_sems, b_sems, w_sems, d_sems, met,
    ) = refs[:7], refs[7:]
    s = lax.axis_index("seq")
    c = lax.axis_index("ch")
    z, y, x, k = s // 4, lax.rem(s, 4), c // 2, lax.rem(c, 2)
    other = 1 - k

    def zdev(mask):
        return {"seq": flip(z, mask) * 4 + y, "ch": c}

    def ydev(mask):
        return {"seq": z * 4 + flip(y, mask), "ch": c}

    def xdev(mask):
        return {"seq": s, "ch": flip(x, mask) * 2 + k}

    partner = {"seq": s, "ch": x * 2 + other}

    def copy(a, b, ss, rs, dev):
        return pltpu.make_async_remote_copy(a, b, ss, rs, device_id=dev, device_id_type=MESH)

    def recv(ref, sem):
        copy(ref, ref, sem, sem, partner).wait_recv()

    def sent(ref, sem):
        copy(ref, ref, sem, sem, partner).wait_send()

    def peers(fn):
        for mask in (2, 1, 3, 0):
            for core in (k, other):
                if mask or core is other:
                    fn(flip(x, mask) * 2 + core)

    copies = [
        pltpu.make_async_copy(a, b, t_sems.at[i])
        for i, (a, b) in enumerate(
            zip(tables_hbm, (first, second, third, last, scatter, regroup, twist))
        )
    ]
    for t in copies:
        t.start()

    barrier = pltpu.get_barrier_semaphore()

    def greet(dev):
        pl.semaphore_signal(barrier, 1, device_id=dev, device_id_type=MESH)

    for mask in (1, 2, 3):
        greet(zdev(mask))
        greet(ydev(mask))
    peers(lambda t: greet({"seq": s, "ch": t}))
    pl.semaphore_wait(barrier, 13)

    class Plane:
        def __init__(self, grab, buf, final, sems):
            self.grab, self.buf, self.final = grab, buf, final
            self.s1, self.s2, self.rfin, self.rbuf = sems

        def dev(self, u, leg, mask):
            return zdev(mask) if u % 2 == leg else ydev(mask)

        def F(self, u):
            for mask in (2, 1, 3):
                if u % 2 == 0:
                    row = self.grab(u, flip(z, mask), slice(None))
                else:
                    row = self.grab(u, slice(None), flip(y, mask))
                to, sem = self.buf.at[u, mask - 1], self.rbuf.at[u, mask - 1]
                copy(row, to, self.s1.at[u], sem, self.dev(u, 0, mask)).start()

        def S(self, u, m1):
            if m1:
                recv(self.buf.at[u, m1 - 1], self.rbuf.at[u, m1 - 1])
            for mask in (2, 1, 3, 0):
                other = flip(y if u % 2 == 0 else z, mask)
                if m1:
                    part = self.buf.at[u, m1 - 1, other]
                else:
                    part = self.grab(u, z, other) if u % 2 == 0 else self.grab(u, other, y)
                if u % 2 == 0:
                    slot = self.final.at[u, flip(z, m1), y]
                else:
                    slot = self.final.at[u, z, flip(y, m1)]
                if mask:
                    to = self.dev(u, 1, mask)
                    copy(part, slot, self.s2.at[u], self.rfin.at[u], to).start()
                else:
                    slot[...] = part[...]

        def done(self, u):
            recv(self.final.at[u, pl.ds(0, 3)], self.rfin.at[u])

        def drain(self, u):
            sent(self.final.at[u, pl.ds(0, 3)], self.s1.at[u])
            sent(self.final.at[u, pl.ds(0, 3)], self.s2.at[u])

    def grab_inputs(u, zi, yi):
        if u < 2:
            return sig.at[zi, yi, u]
        return spec.at[u % 2, zi, yi, u // 2 - 1]

    A = Plane(grab_inputs, buf, final, a_sems)

    def twists(ch):
        on = mode[s * 8 + ch] == 1
        return jnp.where(on, twist[0], 1.0), jnp.where(on, twist[1], 0.0)

    def forward(h, lo):
        def step(m, carry):
            image = final[h, :, :, m].reshape(256, 256)
            value = dot(first[...], image)
            re, im = value[:256], value[256:]
            tc, ts = twists(4 * h + m)
            pair = jnp.concatenate([re * tc + im * ts, im * tc - re * ts], 1).astype(BF16)
            spectral[4 * h + m] = dot(pair, second[...])
            return carry

        lax.fori_loop(lo, lo + 2, step, 0)

    def inverse(h, lo):
        def step(m, carry):
            value = spectral[4 * h + m]
            re, im = value[:, :256], value[:, 256:]
            fr = final[2 + 2 * h, :, :, m].reshape(256, 256).astype(F32)
            fi = final[3 + 2 * h, :, :, m].reshape(256, 256).astype(F32)
            pair = jnp.concatenate([re * fr - im * fi, re * fi + im * fr], 1).astype(BF16)
            value = dot(pair, third[...])
            re, im = value[:, :256], value[:, 256:]
            tc, ts = twists(4 * h + m)
            pair = jnp.concatenate([re * tc - im * ts, re * ts + im * tc], 0).astype(BF16)
            value = dot(last[...], pair)
            image = final[h, :, :, m].reshape(256, 256).astype(F32)
            value = value + gain[s * 8 + 4 * h + m] * image
            hid[m] = value.astype(BF16).reshape(4, 4, 16, 256)
            return carry

        lax.fori_loop(lo, lo + 2, step, 0)

    def place(h):
        for t in range(4):
            block = hid[:, t].reshape(256, 256)
            value = dot(scatter[...], block).astype(BF16)
            send[h, t * 32 : (t + 1) * 32] = value.reshape(32, 8, 256)

    sb, rb = b_sems
    mine = c * 16 + s

    def scatter_all(h):
        def step(i, carry):
            zz, yy = lax.rem(z + lax.rem(i, 4), 4), lax.rem(y + i // 4, 4)
            block = (zz * 4 + yy) * 8
            for mask in (2, 1, 3, 0):
                for core in (k, other):
                    xx = flip(x, mask)
                    part = send.at[h, block + core * 4 + xx]
                    to = {"seq": zz * 4 + yy, "ch": xx * 2 + core}
                    one = copy(part, gathered.at[h, mine], sb.at[h], rb.at[h], to)
                    if mask == 0 and core is k:

                        @pl.when(i > 0)
                        def _():
                            one.start()

                    else:
                        one.start()
            return carry

        lax.fori_loop(0, 16, step, 0)
        gathered[h, mine] = send[h, s * 8 + k * 4 + x]

    own = pl.ds(pl.multiple_of(c * 128, 128), 128)
    ws, wr = w_sems

    def pair(method, u, *m):
        method(u, *m)
        method(u + 1, *m)

    pair(A.F, 0)
    pair(A.F, 2)
    pair(A.S, 0, 0)
    pair(A.S, 2, 0)
    pair(A.F, 4)
    peers(lambda t: copy(w, wfull.at[own], ws, wr, {"seq": s, "ch": t}).start())
    wfull[own] = w[...]
    pair(A.S, 0, 1)
    pair(A.S, 0, 3)
    pair(A.S, 0, 2)
    pair(A.S, 2, 1)
    pair(A.S, 2, 3)
    pair(A.S, 2, 2)
    pair(A.S, 4, 0)
    A.done(0)
    for t in copies:
        t.wait()
    forward(0, 0)
    pair(A.S, 4, 1)
    forward(0, 2)
    A.done(1)
    peers(
        lambda t: pl.semaphore_signal(
            met, 1, device_id={"seq": s, "ch": t}, device_id_type=MESH
        )
    )
    forward(1, 0)
    pair(A.S, 4, 3)
    forward(1, 2)
    pair(A.S, 4, 2)
    A.done(2)
    A.done(3)
    inverse(0, 0)
    inverse(0, 2)
    place(0)
    pl.semaphore_wait(met, 7)
    scatter_all(0)
    A.done(4)
    A.done(5)
    inverse(1, 0)
    inverse(1, 2)
    place(1)
    scatter_all(1)
    recv(wfull.at[pl.ds(0, 7 * 128)], wr)
    recv(gathered.at[0, pl.ds(0, 127)], rb.at[0])
    recv(gathered.at[1, pl.ds(0, 127)], rb.at[1])

    for i in range(8):
        block = jnp.concatenate(
            [gathered[h, 16 * i : 16 * i + 16].reshape(128, 256) for h in range(2)], 0
        )
        value = lax.dot_general(
            block, regroup[...], (((0,), (0,)), ((), ())), preferred_element_type=F32
        ).astype(BF16)
        rows[0, :, i * 128 : (i + 1) * 128] = value[:, :128]
        rows[1, :, i * 128 : (i + 1) * 128] = value[:, 128:]

    for i in range(4):
        value = dot(rows[...].reshape(512, 1024), wfull[:, i * 256 : (i + 1) * 256]).astype(BF16)
        prod[0, i] = value[:, :128]
        prod[1, i] = value[:, 128:]

    ds, dr = d_sems

    def give(t):
        part = prod.at[lax.rem(t, 2), t // 2]
        copy(part, out.at[c], ds, dr, {"seq": s, "ch": t}).start()

    peers(give)
    out[c] = prod[k, x]
    recv(out.at[pl.ds(0, 7)], dr)

    for u in range(6):
        A.drain(u)
    for h in range(2):
        sent(send.at[h, pl.ds(0, 127)], sb.at[h])
    sent(wfull.at[pl.ds(0, 7 * 128)], ws)
    sent(out.at[pl.ds(0, 7)], ds)


def per_device(signal, spectrum, channel_mode, skip_gain, out_weight):
    pieces = signal.reshape(16, 256, 128).astype(BF16).transpose(2, 0, 1)
    pieces = pieces.reshape(4, 4, 2, 4, 16, 256)
    filters = spectrum.astype(BF16).transpose(0, 3, 1, 2)
    filters = filters.reshape(2, 4, 4, 2, 4, 16, 256)
    unit = (4, 16, 256)
    dma = pltpu.SemaphoreType.DMA
    constants = tables()
    anywhere = pl.BlockSpec(memory_space=pltpu.HBM)
    vmem = pl.BlockSpec(memory_space=pltpu.VMEM)
    smem = pl.BlockSpec(memory_space=pltpu.SMEM)
    result = pl.pallas_call(
        kernel,
        out_shape=jax.ShapeDtypeStruct((8, 512, 128), BF16),
        in_specs=[vmem, vmem, vmem, smem, smem] + [anywhere] * 7,
        out_specs=vmem,
        scratch_shapes=[
            *(pltpu.VMEM(t.shape, t.dtype) for t in constants),
            pltpu.VMEM((6, 3, 4) + unit, BF16),
            pltpu.VMEM((6, 4, 4) + unit, BF16),
            pltpu.VMEM((8, 256, 512), F32),
            pltpu.VMEM((4, 4, 4, 16, 256), BF16),
            pltpu.VMEM((2, 128, 8, 256), BF16),
            pltpu.VMEM((2, 128, 8, 256), BF16),
            pltpu.VMEM((2, 256, 1024), BF16),
            pltpu.VMEM((1024, 1024), BF16),
            pltpu.VMEM((2, 4, 512, 128), BF16),
            dma((7,)),
            (dma((6,)), dma((6,)), dma((6,)), dma((6, 3))),
            (dma((2,)), dma((2,))),
            (dma, dma),
            (dma, dma),
            pltpu.SemaphoreType.REGULAR,
        ],
        compiler_params=pltpu.CompilerParams(
            collective_id=0, has_side_effects=True, vmem_limit_bytes=40 << 20
        ),
        name="hyena",
    )(pieces, filters, out_weight, channel_mode, skip_gain, *constants)
    return result.astype(F32).reshape(1, 4096, 128)


def solution(mesh):
    in_specs = (
        P(None, "seq", "ch"), P(None, "seq", None, "ch"), P("ch"), P("ch"), P("ch", None)
    )
    return jax.shard_map(
        per_device, mesh=mesh, in_specs=in_specs, out_specs=P(None, "seq", "ch"), check_vma=False
    )
```

```python
import math

import jax
import jax.numpy as jnp
import numpy as np
from jax import lax
from jax.experimental import pallas as pl
from jax.experimental.pallas import tpu as pltpu
from jax.sharding import PartitionSpec as P

ROWS = 256
COLUMNS = 256
LENGTH = 65536
BF16 = jnp.bfloat16
F32 = jnp.float32
MESH = pl.DeviceIdType.MESH


PITCH = 24


def table():
    counter = np.arange(256)
    product = counter[:, None] * counter[None, :]
    angle = product % 256 * (2.0 * math.pi / 256)
    twist = product * (2.0 * math.pi / LENGTH)
    parts = [np.cos(angle), np.sin(angle), np.cos(twist), np.sin(twist)]
    return jnp.asarray(np.stack(parts), F32)


def flip(v, mask):
    if mask == 0:
        return v
    if mask == 1:
        return v + 1 - 2 * lax.rem(v, 2)
    if mask == 2:
        return lax.rem(v + 2, 4)
    return 3 - v


def dot(a, b):
    return jnp.dot(a, b, preferred_element_type=F32)


def kernel(
    signal, spectrum, w, mode, gain, table_hbm,
    out,
    raw, raw2, turned, sig, spec, twist,
    first, second, third, last, scatter, regroup,
    buf, final, spectral, hid, send, send1, gathered, gathered1, rows, wfull, prod,
    h_sems, a_sems, b_sems, w_sems, d_sems, met,
):
    s = lax.axis_index("seq")
    c = lax.axis_index("ch")
    z, y, x, k = s // 4, lax.rem(s, 4), c // 2, lax.rem(c, 2)
    other = 1 - k

    def zdev(mask):
        return {"seq": flip(z, mask) * 4 + y, "ch": c}

    def ydev(mask):
        return {"seq": z * 4 + flip(y, mask), "ch": c}

    def xdev(mask):
        return {"seq": s, "ch": flip(x, mask) * 2 + k}

    partner = {"seq": s, "ch": x * 2 + other}

    def copy(a, b, ss, rs, dev):
        return pltpu.make_async_remote_copy(a, b, ss, rs, device_id=dev, device_id_type=MESH)

    def recv(ref, sem):
        copy(ref, ref, sem, sem, partner).wait_recv()

    def sent(ref, sem):
        copy(ref, ref, sem, sem, partner).wait_send()

    def peers(fn):
        for mask in (2, 1, 3, 0):
            for core in (k, other):
                if mask or core is other:
                    fn(flip(x, mask) * 2 + core)

    loads = [
        pltpu.make_async_copy(signal.at[pl.ds(4 * i, 4)], raw.at[pl.ds(4 * i, 4)], h_sems.at[i])
        for i in range(4)
    ]
    loads += [
        pltpu.make_async_copy(spectrum.at[i], raw2.at[i], h_sems.at[4 + i]) for i in range(2)
    ]
    loads.append(pltpu.make_async_copy(table_hbm, twist, h_sems.at[6]))
    for load in loads:
        load.start()

    barrier = pltpu.get_barrier_semaphore()

    def greet(dev):
        pl.semaphore_signal(barrier, 1, device_id=dev, device_id_type=MESH)

    for mask in (1, 2, 3):
        greet(zdev(mask))
        greet(ydev(mask))
    peers(lambda t: greet({"seq": s, "ch": t}))

    def turn(source, lo, n):
        def step(a, carry):
            value = source[a].T
            turned.at[0][pl.ds(a, 128, stride=PITCH), :] = value[:, :128]
            turned.at[1][pl.ds(a, 128, stride=PITCH), :] = value[:, 128:]
            return carry

        lax.fori_loop(lo, lo + n, step, 0)

    def pack(target):
        def step(t, carry):
            for h in range(2):
                for m in range(4):
                    at = pl.ds(pl.multiple_of((t * 8 + h * 4 + m) * PITCH, 8), 16)
                    value = jnp.concatenate([turned[0, at, :], turned[1, at, :]], 1)
                    target[t // 4, lax.rem(t, 4), h, m] = value.astype(BF16)
            return carry

        lax.fori_loop(0, 16, step, 0)

    for i in range(4):
        loads[i].wait()
        turn(raw, 4 * i, 4)
    pack(sig)
    pl.semaphore_wait(barrier, 13)

    class Plane:
        def __init__(self, grab, buf, final, sems):
            self.grab, self.buf, self.final = grab, buf, final
            self.s1, self.s2, self.rfin, self.rbuf = sems

        def dev(self, u, leg, mask):
            return zdev(mask) if u % 2 == leg else ydev(mask)

        def F(self, u):
            for mask in (2, 1, 3):
                if u % 2 == 0:
                    row = self.grab(u, flip(z, mask), slice(None))
                else:
                    row = self.grab(u, slice(None), flip(y, mask))
                to, sem = self.buf.at[u, mask - 1], self.rbuf.at[u, mask - 1]
                copy(row, to, self.s1.at[u], sem, self.dev(u, 0, mask)).start()

        def S(self, u, m1):
            if m1:
                recv(self.buf.at[u, m1 - 1], self.rbuf.at[u, m1 - 1])
            for mask in (2, 1, 3, 0):
                other = flip(y if u % 2 == 0 else z, mask)
                if m1:
                    part = self.buf.at[u, m1 - 1, other]
                else:
                    part = self.grab(u, z, other) if u % 2 == 0 else self.grab(u, other, y)
                if u % 2 == 0:
                    slot = self.final.at[u, flip(z, m1), y]
                else:
                    slot = self.final.at[u, z, flip(y, m1)]
                if mask:
                    to = self.dev(u, 1, mask)
                    copy(part, slot, self.s2.at[u], self.rfin.at[u], to).start()
                else:
                    slot[...] = part[...]

        def done(self, u):
            recv(self.final.at[u, pl.ds(0, 3)], self.rfin.at[u])

        def drain(self, u):
            sent(self.final.at[u, pl.ds(0, 3)], self.s1.at[u])
            sent(self.final.at[u, pl.ds(0, 3)], self.s2.at[u])

    def grab_inputs(u, zi, yi):
        if u < 2:
            return sig.at[zi, yi, u]
        return spec.at[u % 2, zi, yi, u // 2 - 1]

    A = Plane(grab_inputs, buf, final, a_sems)

    def twists(ch):
        on = mode[s * 8 + ch] == 1
        return jnp.where(on, twist[2], 1.0), jnp.where(on, twist[3], 0.0)

    def forward(h, lo):
        def step(m, carry):
            image = final[h, :, :, m].reshape(256, 256)
            value = dot(first[...], image)
            re, im = value[:256], value[256:]
            tc, ts = twists(4 * h + m)
            pair = jnp.concatenate([re * tc + im * ts, im * tc - re * ts], 1).astype(BF16)
            spectral[4 * h + m] = dot(pair, second[...])
            return carry

        lax.fori_loop(lo, lo + 2, step, 0)

    def inverse(h, lo):
        def step(m, carry):
            value = spectral[4 * h + m]
            re, im = value[:, :256], value[:, 256:]
            fr = final[2 + 2 * h, :, :, m].reshape(256, 256).astype(F32)
            fi = final[3 + 2 * h, :, :, m].reshape(256, 256).astype(F32)
            pair = jnp.concatenate([re * fr - im * fi, re * fi + im * fr], 1).astype(BF16)
            value = dot(pair, third[...])
            re, im = value[:, :256], value[:, 256:]
            tc, ts = twists(4 * h + m)
            pair = jnp.concatenate([re * tc - im * ts, re * ts + im * tc], 0).astype(BF16)
            value = dot(last[...], pair)
            image = final[h, :, :, m].reshape(256, 256).astype(F32)
            value = value + gain[s * 8 + 4 * h + m] * image
            hid[m] = value.astype(BF16).reshape(4, 4, 16, 256)
            return carry

        lax.fori_loop(lo, lo + 2, step, 0)

    def build():
        cos, sin = twist[0], twist[1]
        first[:256], first[256:] = cos.astype(BF16), (-sin).astype(BF16)
        second[:256, :256] = second[256:, 256:] = cos.astype(BF16)
        third[:256, :256] = third[256:, 256:] = cos.astype(BF16)
        second[:256, 256:] = third[256:, :256] = (-sin).astype(BF16)
        second[256:, :256] = third[:256, 256:] = sin.astype(BF16)
        last[:, :256] = (cos / LENGTH).astype(BF16)
        last[:, 256:] = (-sin / LENGTH).astype(BF16)
        i = lax.broadcasted_iota(jnp.int32, (256, 256), 0)
        j = lax.broadcasted_iota(jnp.int32, (256, 256), 1)
        m, t, at = j >> 6, (j >> 4) & 3, j & 15
        row = t * 64 + ((at >> 1) & 1) * 32 + (at >> 2) * 8 + (at & 1) * 4 + m
        scatter[...] = jnp.where(i == row, 1.0, 0.0).astype(BF16)
        column = ((i >> 2) & 1) * 128 + ((i >> 3) & 15) * 8 + (i >> 7) * 4 + (i & 3)
        regroup[...] = jnp.where(j == column, 1.0, 0.0).astype(BF16)

    def place(h):
        for t in range(4):
            block = hid[:, t].reshape(256, 256)
            value = dot(scatter[...], block).astype(BF16)
            if h == 0:
                send[t * 32 : (t + 1) * 32] = value.reshape(32, 8, 256)
            else:
                for e in range(2):
                    part = value[:, e * 128 : (e + 1) * 128]
                    send1[e, t * 32 : (t + 1) * 32] = part.reshape(32, 8, 128)

    sb, rb = b_sems
    mine = c * 16 + s

    def scatter_all(source, target, i_sem):
        def step(i, carry):
            zz, yy = lax.rem(z + lax.rem(i, 4), 4), lax.rem(y + i // 4, 4)
            block = (zz * 4 + yy) * 8
            for mask in (2, 1, 3, 0):
                for core in (k, other):
                    xx = flip(x, mask)
                    part = source.at[block + core * 4 + xx]
                    to = {"seq": zz * 4 + yy, "ch": xx * 2 + core}
                    one = copy(part, target.at[mine], sb.at[i_sem], rb.at[i_sem], to)
                    if mask == 0 and core is k:

                        @pl.when(i > 0)
                        def _():
                            one.start()

                    else:
                        one.start()
            return carry

        lax.fori_loop(0, 16, step, 0)
        target[mine] = source[s * 8 + k * 4 + x]

    own = pl.ds(pl.multiple_of(c * 128, 128), 128)
    ws, wr = w_sems

    def pair(method, u, *m):
        method(u, *m)
        method(u + 1, *m)

    pair(A.F, 0)
    pair(A.S, 0, 0)
    for i in range(2):
        loads[4 + i].wait()
        turn(raw2.at[i], 0, 16)
        pack(spec.at[i])
        A.F(2 + i)
    pair(A.S, 0, 1)
    pair(A.S, 0, 3)
    pair(A.S, 2, 0)
    peers(lambda t: copy(w, wfull.at[own], ws, wr, {"seq": s, "ch": t}).start())
    wfull[own] = w[...]
    pair(A.S, 0, 2)
    pair(A.F, 4)
    loads[6].wait()
    build()
    pair(A.S, 2, 1)
    pair(A.S, 2, 3)
    pair(A.S, 2, 2)
    pair(A.S, 4, 0)
    A.done(0)
    forward(0, 0)
    forward(0, 2)
    A.done(1)
    peers(
        lambda t: pl.semaphore_signal(
            met, 1, device_id={"seq": s, "ch": t}, device_id_type=MESH
        )
    )
    pair(A.S, 4, 1)
    forward(1, 0)
    pair(A.S, 4, 3)
    forward(1, 2)
    pair(A.S, 4, 2)
    A.done(2)
    A.done(3)
    inverse(0, 0)
    inverse(0, 2)
    place(0)
    pl.semaphore_wait(met, 7)
    scatter_all(send, gathered, 0)
    A.done(4)
    A.done(5)
    inverse(1, 0)
    inverse(1, 2)
    place(1)
    scatter_all(send1.at[0], gathered1.at[0], 1)
    scatter_all(send1.at[1], gathered1.at[1], 2)
    recv(wfull.at[pl.ds(0, 7 * 128)], wr)
    recv(gathered.at[pl.ds(0, 127)], rb.at[0])

    ds, dr = d_sems

    def project(e):
        recv(gathered1.at[e, pl.ds(0, 127)], rb.at[1 + e])
        for i in range(8):
            old = gathered[16 * i : 16 * i + 16, :, e * 128 : (e + 1) * 128].reshape(128, 128)
            new = gathered1[e, 16 * i : 16 * i + 16].reshape(128, 128)
            value = lax.dot_general(
                jnp.concatenate([old, new], 0),
                regroup[...],
                (((0,), (0,)), ((), ())),
                preferred_element_type=F32,
            ).astype(BF16)
            rows[:128, i * 128 : (i + 1) * 128] = value[:, :128]
            rows[128:, i * 128 : (i + 1) * 128] = value[:, 128:]
        for mask in (2, 1, 3, 0):
            xx = flip(x, mask)
            columns = wfull[:, pl.ds(pl.multiple_of(xx * 256, 256), 256)]
            value = dot(rows[...], columns).astype(BF16)
            for core in range(2):
                part = value[:, core * 128 : (core + 1) * 128]
                prod[e, xx * 2 + core] = part.reshape(2, 128, 128)
            for core in (k, other):
                if mask or core is other:
                    to = {"seq": s, "ch": xx * 2 + core}
                    part = prod.at[e, xx * 2 + core]
                    copy(part, out.at[c, :, e], ds.at[e], dr.at[e], to).start()
        out[c, :, e] = prod[e, c]

    project(0)
    project(1)
    for e in range(2):
        recv(prod.at[e, pl.ds(0, 7)], dr.at[e])

    for u in range(6):
        A.drain(u)
    sent(send.at[pl.ds(0, 127)], sb.at[0])
    for e in range(2):
        sent(send1.at[e, pl.ds(0, 127)], sb.at[1 + e])
        sent(prod.at[e, pl.ds(0, 7)], ds.at[e])
    sent(wfull.at[pl.ds(0, 7 * 128)], ws)


def per_device(signal, spectrum, channel_mode, skip_gain, out_weight):
    unit = (4, 16, 256)
    dma = pltpu.SemaphoreType.DMA
    constant = table()
    vmem = pl.BlockSpec(memory_space=pltpu.VMEM)
    smem = pl.BlockSpec(memory_space=pltpu.SMEM)
    hbm = pl.BlockSpec(memory_space=pltpu.HBM)
    result = pl.pallas_call(
        kernel,
        out_shape=jax.ShapeDtypeStruct((8, 2, 2, 128, 128), BF16),
        in_specs=[hbm, hbm, vmem, smem, smem, hbm],
        out_specs=vmem,
        scratch_shapes=[
            pltpu.VMEM((16, 256, 128), F32),
            pltpu.VMEM((2, 16, 256, 128), F32),
            pltpu.VMEM((2, 128 * PITCH, 128), F32),
            pltpu.VMEM((4, 4, 2) + unit, BF16),
            pltpu.VMEM((2, 4, 4, 2) + unit, BF16),
            pltpu.VMEM((4, 256, 256), F32),
            pltpu.VMEM((512, 256), BF16),
            pltpu.VMEM((512, 512), BF16),
            pltpu.VMEM((512, 512), BF16),
            pltpu.VMEM((256, 512), BF16),
            pltpu.VMEM((256, 256), BF16),
            pltpu.VMEM((256, 256), BF16),
            pltpu.VMEM((6, 3, 4) + unit, BF16),
            pltpu.VMEM((6, 4, 4) + unit, BF16),
            pltpu.VMEM((8, 256, 512), F32),
            pltpu.VMEM((4, 4, 4, 16, 256), BF16),
            pltpu.VMEM((128, 8, 256), BF16),
            pltpu.VMEM((2, 128, 8, 128), BF16),
            pltpu.VMEM((128, 8, 256), BF16),
            pltpu.VMEM((2, 128, 8, 128), BF16),
            pltpu.VMEM((256, 1024), BF16),
            pltpu.VMEM((1024, 1024), BF16),
            pltpu.VMEM((2, 8, 2, 128, 128), BF16),
            dma((7,)),
            (dma((6,)), dma((6,)), dma((6,)), dma((6, 3))),
            (dma((3,)), dma((3,))),
            (dma, dma),
            (dma((2,)), dma((2,))),
            pltpu.SemaphoreType.REGULAR,
        ],
        compiler_params=pltpu.CompilerParams(
            collective_id=0, has_side_effects=True, vmem_limit_bytes=60 << 20
        ),
        name="hyena",
    )(
        signal.reshape(16, 256, 128), spectrum, out_weight, channel_mode, skip_gain, constant
    )
    return result.astype(F32).reshape(1, 4096, 128)


def solution(mesh):
    in_specs = (
        P(None, "seq", "ch"), P(None, "seq", None, "ch"), P("ch"), P("ch"), P("ch", None)
    )
    return jax.shard_map(
        per_device, mesh=mesh, in_specs=in_specs, out_specs=P(None, "seq", "ch"), check_vma=False
    )
```

```python
import math

import jax
import jax.numpy as jnp
import numpy as np
from jax import lax
from jax.experimental import pallas as pl
from jax.experimental.pallas import tpu as pltpu
from jax.sharding import PartitionSpec as P

ROWS = 256
COLUMNS = 256
LENGTH = 65536
BF16 = jnp.bfloat16
F32 = jnp.float32
MESH = pl.DeviceIdType.MESH


PITCH = 24


def table():
    counter = np.arange(256)
    product = counter[:, None] * counter[None, :]
    angle = product % 256 * (2.0 * math.pi / 256)
    twist = product * (2.0 * math.pi / LENGTH)
    parts = [np.cos(angle), np.sin(angle), np.cos(twist), np.sin(twist)]
    return jnp.asarray(np.stack(parts), F32)


def flip(v, mask):
    if mask == 0:
        return v
    if mask == 1:
        return v + 1 - 2 * lax.rem(v, 2)
    if mask == 2:
        return lax.rem(v + 2, 4)
    return 3 - v


def dot(a, b):
    return jnp.dot(a, b, preferred_element_type=F32)


def flip2(v, step):
    return lax.rem(v + jnp.where(step == 3, 2, jnp.where(step == 2, 3, step)), 4)


def kernel(
    signal, spectrum, w_hbm, mode_hbm, gain_hbm, table_hbm,
    out,
    raw, raw2, turned, sig, spec, twist, w, mode, gain,
    first, second, third, last, scatter, regroup, order,
    buf, final, spectral, hid, send, gathered, rows, total, wmine, wfull, prod,
    h_sems, a_sems, b_sems, w_sems, d_sems, met,
):
    s = lax.axis_index("seq")
    c = lax.axis_index("ch")
    z, y, x, k = s // 4, lax.rem(s, 4), c // 2, lax.rem(c, 2)
    other = 1 - k

    def zdev(mask):
        return {"seq": flip(z, mask) * 4 + y, "ch": c}

    def ydev(mask):
        return {"seq": z * 4 + flip(y, mask), "ch": c}

    def xdev(mask):
        return {"seq": s, "ch": flip(x, mask) * 2 + k}

    partner = {"seq": s, "ch": x * 2 + other}

    def copy(a, b, ss, rs, dev):
        return pltpu.make_async_remote_copy(a, b, ss, rs, device_id=dev, device_id_type=MESH)

    def recv(ref, sem):
        copy(ref, ref, sem, sem, partner).wait_recv()

    def sent(ref, sem):
        copy(ref, ref, sem, sem, partner).wait_send()

    def peers(fn):
        for mask in (2, 1, 3, 0):
            for core in (k, other):
                if mask or core is other:
                    fn(flip(x, mask) * 2 + core)

    loads = [
        pltpu.make_async_copy(signal.at[pl.ds(4 * i, 4)], raw.at[pl.ds(4 * i, 4)], h_sems.at[i])
        for i in range(4)
    ]
    loads += [
        pltpu.make_async_copy(spectrum.at[i], raw2.at[i], h_sems.at[4 + i]) for i in range(2)
    ]
    small = ((table_hbm, twist), (w_hbm, w), (mode_hbm, mode), (gain_hbm, gain))
    for i, (a, b) in enumerate(small):
        loads.append(pltpu.make_async_copy(a, b, h_sems.at[6 + i]))
    for load in loads:
        load.start()

    barrier = pltpu.get_barrier_semaphore()

    def greet(dev):
        pl.semaphore_signal(barrier, 1, device_id=dev, device_id_type=MESH)

    for mask in (1, 2, 3):
        greet(zdev(mask))
        greet(ydev(mask))
    peers(lambda t: greet({"seq": s, "ch": t}))

    def turn(source, lo, n):
        def step(a, carry):
            value = source[a].T
            turned.at[0][pl.ds(a, 128, stride=PITCH), :] = value[:, :128]
            turned.at[1][pl.ds(a, 128, stride=PITCH), :] = value[:, 128:]
            return carry

        lax.fori_loop(lo, lo + n, step, 0)

    def pack(target):
        def step(t, carry):
            for h in range(2):
                for m in range(4):
                    at = pl.ds(pl.multiple_of((t * 8 + h * 4 + m) * PITCH, 8), 16)
                    value = jnp.concatenate([turned[0, at, :], turned[1, at, :]], 1)
                    target[t // 4, lax.rem(t, 4), h, m] = value.astype(BF16)
            return carry

        lax.fori_loop(0, 16, step, 0)

    for i in range(4):
        loads[i].wait()
        turn(raw, 4 * i, 4)
    pack(sig)
    pl.semaphore_wait(barrier, 13)

    class Plane:
        def __init__(self, grab, buf, final, sems):
            self.grab, self.buf, self.final = grab, buf, final
            self.s1, self.s2, self.rfin, self.rbuf = sems

        def dev(self, u, leg, mask):
            return zdev(mask) if u % 2 == leg else ydev(mask)

        def F(self, u):
            for mask in (2, 1, 3):
                if u % 2 == 0:
                    row = self.grab(u, flip(z, mask), slice(None))
                else:
                    row = self.grab(u, slice(None), flip(y, mask))
                to, sem = self.buf.at[u, mask - 1], self.rbuf.at[u, mask - 1]
                copy(row, to, self.s1.at[u], sem, self.dev(u, 0, mask)).start()

        def S(self, u, m1):
            if m1:
                recv(self.buf.at[u, m1 - 1], self.rbuf.at[u, m1 - 1])
            for mask in (2, 1, 3, 0):
                other = flip(y if u % 2 == 0 else z, mask)
                if m1:
                    part = self.buf.at[u, m1 - 1, other]
                else:
                    part = self.grab(u, z, other) if u % 2 == 0 else self.grab(u, other, y)
                if u % 2 == 0:
                    slot = self.final.at[u, flip(z, m1), y]
                else:
                    slot = self.final.at[u, z, flip(y, m1)]
                if mask:
                    to = self.dev(u, 1, mask)
                    copy(part, slot, self.s2.at[u], self.rfin.at[u], to).start()
                else:
                    slot[...] = part[...]

        def done(self, u):
            recv(self.final.at[u, pl.ds(0, 3)], self.rfin.at[u])

        def drain(self, u):
            sent(self.final.at[u, pl.ds(0, 3)], self.s1.at[u])
            sent(self.final.at[u, pl.ds(0, 3)], self.s2.at[u])

    def grab_inputs(u, zi, yi):
        if u < 2:
            return sig.at[zi, yi, u]
        return spec.at[u % 2, zi, yi, u // 2 - 1]

    A = Plane(grab_inputs, buf, final, a_sems)

    def twists(ch):
        on = mode[s * 8 + ch] == 1
        return jnp.where(on, twist[2], 1.0), jnp.where(on, twist[3], 0.0)

    def forward(h, lo):
        def step(m, carry):
            image = final[h, :, :, m].reshape(256, 256)
            value = dot(first[...], image)
            re, im = value[:256], value[256:]
            tc, ts = twists(4 * h + m)
            pair = jnp.concatenate([re * tc + im * ts, im * tc - re * ts], 1).astype(BF16)
            spectral[4 * h + m] = dot(pair, second[...])
            return carry

        lax.fori_loop(lo, lo + 2, step, 0, unroll=True)

    def inverse(h, lo):
        def step(m, carry):
            value = spectral[4 * h + m]
            re, im = value[:, :256], value[:, 256:]
            fr = final[2 + 2 * h, :, :, m].reshape(256, 256).astype(F32)
            fi = final[3 + 2 * h, :, :, m].reshape(256, 256).astype(F32)
            pair = jnp.concatenate([re * fr - im * fi, re * fi + im * fr], 1).astype(BF16)
            value = dot(pair, third[...])
            re, im = value[:, :256], value[:, 256:]
            tc, ts = twists(4 * h + m)
            pair = jnp.concatenate([re * tc - im * ts, re * ts + im * tc], 0).astype(BF16)
            value = dot(last[...], pair)
            image = final[h, :, :, m].reshape(256, 256).astype(F32)
            value = value + gain[s * 8 + 4 * h + m] * image
            hid[m] = value.astype(BF16).reshape(4, 4, 16, 256)
            return carry

        lax.fori_loop(lo, lo + 2, step, 0, unroll=True)

    def build():
        cos, sin = twist[0], twist[1]
        first[:256], first[256:] = cos.astype(BF16), (-sin).astype(BF16)
        second[:256, :256] = second[256:, 256:] = cos.astype(BF16)
        third[:256, :256] = third[256:, 256:] = cos.astype(BF16)
        second[:256, 256:] = third[256:, :256] = (-sin).astype(BF16)
        second[256:, :256] = third[:256, 256:] = sin.astype(BF16)
        last[:, :256] = (cos / LENGTH).astype(BF16)
        last[:, 256:] = (-sin / LENGTH).astype(BF16)
        i = lax.broadcasted_iota(jnp.int32, (256, 256), 0)
        j = lax.broadcasted_iota(jnp.int32, (256, 256), 1)
        m, t, at = j >> 6, (j >> 4) & 3, j & 15
        row = t * 64 + ((at >> 1) & 1) * 32 + (at >> 2) * 8 + (at & 1) * 4 + m
        scatter[...] = jnp.where(i == row, 1.0, 0.0).astype(BF16)
        column = ((i >> 2) & 1) * 128 + (i >> 7) * 64 + ((i >> 3) & 15) * 4 + (i & 3)
        regroup[...] = jnp.where(j == column, 1.0, 0.0).astype(BF16)
        i, j = i[:128, :128], j[:128, :128]
        row = ((j >> 2) & 1) * 64 + (j >> 3) * 4 + (j & 3)
        order[...] = jnp.where(i == row, 1.0, 0.0).astype(BF16)

    def place(h):
        for t in range(4):
            block = hid[:, t].reshape(256, 256)
            value = dot(scatter[...], block).astype(BF16)
            for e in range(2):
                part = value[:, e * 128 : (e + 1) * 128]
                send[h, e, t * 32 : (t + 1) * 32] = part.reshape(32, 8, 128)

    sb, rb = b_sems
    mine = c * 16 + s

    def scatter_all(h, e):
        source, target = send.at[h, e], gathered.at[h, e]
        sem, done = sb.at[h, e], rb.at[h, e]

        def step(i, carry):
            i = 15 - i
            zz, yy = flip2(z, lax.rem(i, 4)), flip2(y, i // 4)
            block = (zz * 4 + yy) * 8
            for mask in (2, 1, 3, 0):
                for core in (k, other):
                    xx = flip(x, mask)
                    part = source.at[block + core * 4 + xx]
                    to = {"seq": zz * 4 + yy, "ch": xx * 2 + core}
                    one = copy(part, target.at[mine], sem, done, to)
                    if mask == 0 and core is k:

                        @pl.when(i > 0)
                        def _():
                            one.start()

                    else:
                        one.start()
            return carry

        lax.fori_loop(0, 16, step, 0)
        target[mine] = source[s * 8 + k * 4 + x]

    ws, wr = w_sems

    def pair(method, u, *m):
        method(u, *m)
        method(u + 1, *m)

    pair(A.F, 0)
    pair(A.S, 0, 0)
    for i in range(2):
        loads[4 + i].wait()
        turn(raw2.at[i], 0, 16)
        pack(spec.at[i])
        A.F(2 + i)
    pair(A.S, 0, 1)
    pair(A.S, 0, 3)
    pair(A.S, 2, 0)
    for i in (6, 7, 8, 9):
        loads[i].wait()
    build()
    wmine[...] = dot(order[...], w[...]).astype(BF16).reshape(2, 64, 1024)
    peers(lambda t: copy(wmine, wfull.at[:, c], ws, wr, {"seq": s, "ch": t}).start())
    wfull[:, c] = wmine[...]
    pair(A.S, 0, 2)
    pair(A.F, 4)
    pair(A.S, 2, 1)
    pair(A.S, 2, 3)
    pair(A.S, 2, 2)
    pair(A.S, 4, 0)
    A.done(0)
    forward(0, 0)
    forward(0, 2)
    A.done(1)
    peers(
        lambda t: pl.semaphore_signal(
            met, 1, device_id={"seq": s, "ch": t}, device_id_type=MESH
        )
    )
    pair(A.S, 4, 1)
    forward(1, 0)
    pair(A.S, 4, 3)
    forward(1, 2)
    pair(A.S, 4, 2)
    A.done(2)
    A.done(3)
    inverse(0, 0)
    inverse(0, 2)
    place(0)
    pl.semaphore_wait(met, 7)
    scatter_all(0, 0)
    A.done(4)
    A.done(5)
    inverse(1, 0)
    inverse(1, 2)
    place(1)
    scatter_all(1, 0)
    scatter_all(0, 1)
    scatter_all(1, 1)
    recv(wfull.at[:, pl.ds(0, 7)], wr)

    ds, dr = d_sems

    def arrange(h, e):
        recv(gathered.at[h, e, pl.ds(0, 127)], rb.at[h, e])
        for i in range(4):
            value = lax.dot_general(
                gathered[h, e, 32 * i : 32 * i + 32].reshape(256, 128),
                regroup[...],
                (((0,), (0,)), ((), ())),
                preferred_element_type=F32,
            ).astype(BF16)
            rows[:128, i * 128 : (i + 1) * 128] = value[:, :128]
            rows[128:, i * 128 : (i + 1) * 128] = value[:, 128:]

    def begin(e):
        arrange(0, e)
        total[...] = dot(rows[...], wfull[0].reshape(512, 1024))

    def finish(e):
        arrange(1, e)
        for mask in (2, 1, 3, 0):
            xx = flip(x, mask)
            columns = pl.ds(pl.multiple_of(xx * 256, 256), 256)
            value = dot(rows[...], wfull[1, :, :, columns].reshape(512, 256))
            value = (total[:, columns] + value).astype(BF16)
            for core in range(2):
                part = value[:, core * 128 : (core + 1) * 128]
                prod[e, xx * 2 + core] = part.reshape(2, 128, 128)
            for core in (k, other):
                if mask or core is other:
                    to = {"seq": s, "ch": xx * 2 + core}
                    part = prod.at[e, xx * 2 + core]
                    copy(part, out.at[c, :, e], ds.at[e], dr.at[e], to).start()
        out[c, :, e] = prod[e, c]

    begin(0)
    finish(0)
    begin(1)
    finish(1)
    for e in range(2):
        recv(prod.at[e, pl.ds(0, 7)], dr.at[e])

    for u in range(6):
        A.drain(u)
    for e in range(2):
        for h in range(2):
            sent(send.at[h, e, pl.ds(0, 127)], sb.at[h, e])
        sent(prod.at[e, pl.ds(0, 7)], ds.at[e])
    sent(wfull.at[:, pl.ds(0, 7)], ws)


def per_device(signal, spectrum, channel_mode, skip_gain, out_weight):
    unit = (4, 16, 256)
    dma = pltpu.SemaphoreType.DMA
    constant = table()
    vmem = pl.BlockSpec(memory_space=pltpu.VMEM)
    hbm = pl.BlockSpec(memory_space=pltpu.HBM)
    fixed = [
        pltpu.with_memory_space_constraint(t, pltpu.HBM)
        for t in (out_weight, channel_mode, skip_gain)
    ]
    result = pl.pallas_call(
        kernel,
        out_shape=jax.ShapeDtypeStruct((8, 2, 2, 128, 128), BF16),
        in_specs=[hbm] * 6,
        out_specs=vmem,
        scratch_shapes=[
            pltpu.VMEM((16, 256, 128), F32),
            pltpu.VMEM((2, 16, 256, 128), F32),
            pltpu.VMEM((2, 128 * PITCH, 128), F32),
            pltpu.VMEM((4, 4, 2) + unit, BF16),
            pltpu.VMEM((2, 4, 4, 2) + unit, BF16),
            pltpu.VMEM((4, 256, 256), F32),
            pltpu.VMEM((128, 1024), BF16),
            pltpu.SMEM((128,), jnp.int32),
            pltpu.SMEM((128,), F32),
            pltpu.VMEM((512, 256), BF16),
            pltpu.VMEM((512, 512), BF16),
            pltpu.VMEM((512, 512), BF16),
            pltpu.VMEM((256, 512), BF16),
            pltpu.VMEM((256, 256), BF16),
            pltpu.VMEM((256, 256), BF16),
            pltpu.VMEM((128, 128), BF16),
            pltpu.VMEM((6, 3, 4) + unit, BF16),
            pltpu.VMEM((6, 4, 4) + unit, BF16),
            pltpu.VMEM((8, 256, 512), F32),
            pltpu.VMEM((4, 4, 4, 16, 256), BF16),
            pltpu.VMEM((2, 2, 128, 8, 128), BF16),
            pltpu.VMEM((2, 2, 128, 8, 128), BF16),
            pltpu.VMEM((256, 512), BF16),
            pltpu.VMEM((256, 1024), F32),
            pltpu.VMEM((2, 64, 1024), BF16),
            pltpu.VMEM((2, 8, 64, 1024), BF16),
            pltpu.VMEM((2, 8, 2, 128, 128), BF16),
            dma((10,)),
            (dma((6,)), dma((6,)), dma((6,)), dma((6, 3))),
            (dma((2, 2)), dma((2, 2))),
            (dma, dma),
            (dma((2,)), dma((2,))),
            pltpu.SemaphoreType.REGULAR,
        ],
        compiler_params=pltpu.CompilerParams(
            collective_id=0, has_side_effects=True, vmem_limit_bytes=52 << 20
        ),
        name="hyena",
    )(
        signal.reshape(16, 256, 128), spectrum, *fixed, constant
    )
    return result.astype(F32).reshape(1, 4096, 128)


def solution(mesh):
    in_specs = (
        P(None, "seq", "ch"), P(None, "seq", None, "ch"), P("ch"), P("ch"), P("ch", None)
    )
    return jax.shard_map(
        per_device, mesh=mesh, in_specs=in_specs, out_specs=P(None, "seq", "ch"), check_vma=False
    )
```

```python
import math

import jax
import jax.numpy as jnp
import numpy as np
from jax import lax
from jax.experimental import pallas as pl
from jax.experimental.pallas import tpu as pltpu
from jax.sharding import PartitionSpec as P

ROWS = 256
COLUMNS = 256
LENGTH = 65536
BF16 = jnp.bfloat16
F32 = jnp.float32
MESH = pl.DeviceIdType.MESH


PITCH = 24


def table():
    counter = np.arange(256)
    product = counter[:, None] * counter[None, :]
    angle = product % 256 * (2.0 * math.pi / 256)
    twist = product * (2.0 * math.pi / LENGTH)
    parts = [np.cos(angle), np.sin(angle), np.cos(twist), np.sin(twist)]
    return jnp.asarray(np.stack(parts), F32)


def flip(v, mask):
    if mask == 0:
        return v
    if mask == 1:
        return v + 1 - 2 * lax.rem(v, 2)
    if mask == 2:
        return lax.rem(v + 2, 4)
    return 3 - v


def dot(a, b):
    return jnp.dot(a, b, preferred_element_type=F32)


def flip2(v, step):
    return lax.rem(v + jnp.where(step == 3, 2, jnp.where(step == 2, 3, step)), 4)


def kernel(
    signal, spectrum, w_hbm, mode_hbm, gain_hbm, table_hbm,
    out,
    raw, raw2, turned, sig, spec, twist, w, mode, gain,
    first, second, third, last, scatter, regroup, order,
    buf, final, spectral, hid, send, gathered, rows, total, wmine, wfull, prod,
    h_sems, a_sems, b_sems, w_sems, d_sems, met,
):
    s = lax.axis_index("seq")
    c = lax.axis_index("ch")
    z, y, x, k = s // 4, lax.rem(s, 4), c // 2, lax.rem(c, 2)
    other = 1 - k

    def zdev(mask):
        return {"seq": flip(z, mask) * 4 + y, "ch": c}

    def ydev(mask):
        return {"seq": z * 4 + flip(y, mask), "ch": c}

    def xdev(mask):
        return {"seq": s, "ch": flip(x, mask) * 2 + k}

    partner = {"seq": s, "ch": x * 2 + other}

    def copy(a, b, ss, rs, dev):
        return pltpu.make_async_remote_copy(a, b, ss, rs, device_id=dev, device_id_type=MESH)

    def recv(ref, sem):
        copy(ref, ref, sem, sem, partner).wait_recv()

    def sent(ref, sem):
        copy(ref, ref, sem, sem, partner).wait_send()

    def peers(fn):
        for mask in (2, 1, 3, 0):
            for core in (k, other):
                if mask or core is other:
                    fn(flip(x, mask) * 2 + core)

    loads = [
        pltpu.make_async_copy(signal.at[pl.ds(4 * i, 4)], raw.at[pl.ds(4 * i, 4)], h_sems.at[i])
        for i in range(4)
    ]
    loads += [
        pltpu.make_async_copy(spectrum.at[i], raw2.at[i], h_sems.at[4 + i]) for i in range(2)
    ]
    small = ((table_hbm, twist), (w_hbm, w), (mode_hbm, mode), (gain_hbm, gain))
    for i, (a, b) in enumerate(small):
        loads.append(pltpu.make_async_copy(a, b, h_sems.at[6 + i]))
    for load in loads:
        load.start()

    barrier = pltpu.get_barrier_semaphore()

    def greet(dev):
        pl.semaphore_signal(barrier, 1, device_id=dev, device_id_type=MESH)

    for mask in (1, 2, 3):
        greet(zdev(mask))
        greet(ydev(mask))
    peers(lambda t: greet({"seq": s, "ch": t}))

    def turn(source, lo, n):
        def step(a, carry):
            value = source[a].T
            turned.at[0][pl.ds(a, 128, stride=PITCH), :] = value[:, :128]
            turned.at[1][pl.ds(a, 128, stride=PITCH), :] = value[:, 128:]
            return carry

        lax.fori_loop(lo, lo + n, step, 0, unroll=4)

    def pack(target):
        def step(t, carry):
            for h in range(2):
                for m in range(4):
                    at = pl.ds(pl.multiple_of((t * 8 + h * 4 + m) * PITCH, 8), 16)
                    value = jnp.concatenate([turned[0, at, :], turned[1, at, :]], 1)
                    target[t // 4, lax.rem(t, 4), h, m] = value.astype(BF16)
            return carry

        lax.fori_loop(0, 16, step, 0)

    for i in range(4):
        loads[i].wait()
        turn(raw, 4 * i, 4)
    pack(sig)
    pl.semaphore_wait(barrier, 13)

    class Plane:
        def __init__(self, grab, buf, final, sems):
            self.grab, self.buf, self.final = grab, buf, final
            self.s1, self.s2, self.rfin, self.rbuf = sems

        def dev(self, u, leg, mask):
            return zdev(mask) if u % 2 == leg else ydev(mask)

        def F(self, u):
            for mask in (2, 1, 3):
                if u % 2 == 0:
                    row = self.grab(u, flip(z, mask), slice(None))
                else:
                    row = self.grab(u, slice(None), flip(y, mask))
                to, sem = self.buf.at[u, mask - 1], self.rbuf.at[u, mask - 1]
                copy(row, to, self.s1.at[u], sem, self.dev(u, 0, mask)).start()

        def S(self, u, m1):
            if m1:
                recv(self.buf.at[u, m1 - 1], self.rbuf.at[u, m1 - 1])
            for mask in (2, 1, 3, 0):
                other = flip(y if u % 2 == 0 else z, mask)
                if m1:
                    part = self.buf.at[u, m1 - 1, other]
                else:
                    part = self.grab(u, z, other) if u % 2 == 0 else self.grab(u, other, y)
                if u % 2 == 0:
                    slot = self.final.at[u, flip(z, m1), y]
                else:
                    slot = self.final.at[u, z, flip(y, m1)]
                if mask:
                    to = self.dev(u, 1, mask)
                    copy(part, slot, self.s2.at[u], self.rfin.at[u], to).start()
                else:
                    slot[...] = part[...]

        def done(self, u):
            recv(self.final.at[u, pl.ds(0, 3)], self.rfin.at[u])

        def drain(self, u):
            sent(self.final.at[u, pl.ds(0, 3)], self.s1.at[u])
            sent(self.final.at[u, pl.ds(0, 3)], self.s2.at[u])

    def grab_inputs(u, zi, yi):
        if u < 2:
            return sig.at[zi, yi, u]
        return spec.at[u % 2, zi, yi, u // 2 - 1]

    A = Plane(grab_inputs, buf, final, a_sems)

    def twists(ch):
        on = mode[s * 8 + ch] == 1
        return jnp.where(on, twist[2], 1.0), jnp.where(on, twist[3], 0.0)

    def forward(h, lo):
        def step(m, carry):
            image = final[h, :, :, m].reshape(256, 256)
            value = dot(first[...], image)
            re, im = value[:256], value[256:]
            tc, ts = twists(4 * h + m)
            pair = jnp.concatenate([re * tc + im * ts, im * tc - re * ts], 1).astype(BF16)
            spectral[4 * h + m] = dot(pair, second[...])
            return carry

        lax.fori_loop(lo, lo + 2, step, 0, unroll=True)

    def inverse(h, lo):
        def step(m, carry):
            value = spectral[4 * h + m]
            re, im = value[:, :256], value[:, 256:]
            fr = final[2 + 2 * h, :, :, m].reshape(256, 256).astype(F32)
            fi = final[3 + 2 * h, :, :, m].reshape(256, 256).astype(F32)
            pair = jnp.concatenate([re * fr - im * fi, re * fi + im * fr], 1).astype(BF16)
            value = dot(pair, third[...])
            re, im = value[:, :256], value[:, 256:]
            tc, ts = twists(4 * h + m)
            pair = jnp.concatenate([re * tc - im * ts, re * ts + im * tc], 0).astype(BF16)
            value = dot(last[...], pair)
            image = final[h, :, :, m].reshape(256, 256).astype(F32)
            value = value + gain[s * 8 + 4 * h + m] * image
            hid[m] = value.astype(BF16).reshape(4, 4, 16, 256)
            return carry

        lax.fori_loop(lo, lo + 2, step, 0, unroll=True)

    def build():
        cos, sin = twist[0], twist[1]
        first[:256], first[256:] = cos.astype(BF16), (-sin).astype(BF16)
        second[:256, :256] = second[256:, 256:] = cos.astype(BF16)
        third[:256, :256] = third[256:, 256:] = cos.astype(BF16)
        second[:256, 256:] = third[256:, :256] = (-sin).astype(BF16)
        second[256:, :256] = third[:256, 256:] = sin.astype(BF16)
        last[:, :256] = (cos / LENGTH).astype(BF16)
        last[:, 256:] = (-sin / LENGTH).astype(BF16)
        i = lax.broadcasted_iota(jnp.int32, (256, 256), 0)
        j = lax.broadcasted_iota(jnp.int32, (256, 256), 1)
        m, t, at = j >> 6, (j >> 4) & 3, j & 15
        row = t * 64 + ((at >> 1) & 1) * 32 + (at >> 2) * 8 + (at & 1) * 4 + m
        scatter[...] = jnp.where(i == row, 1.0, 0.0).astype(BF16)
        column = ((i >> 2) & 1) * 128 + (i >> 7) * 64 + ((i >> 3) & 15) * 4 + (i & 3)
        regroup[...] = jnp.where(j == column, 1.0, 0.0).astype(BF16)
        i, j = i[:128, :128], j[:128, :128]
        row = ((j >> 2) & 1) * 64 + (j >> 3) * 4 + (j & 3)
        order[...] = jnp.where(i == row, 1.0, 0.0).astype(BF16)

    def place(h):
        for t in range(4):
            block = hid[:, t].reshape(256, 256)
            value = dot(scatter[...], block).astype(BF16)
            for e in range(2):
                part = value[:, e * 128 : (e + 1) * 128]
                send[h, e, t * 32 : (t + 1) * 32] = part.reshape(32, 8, 128)

    sb, rb = b_sems
    mine = c * 16 + s

    def scatter_to(core, h, e):
        source, target = send.at[h, e], gathered.at[h, e]
        sem, done = sb.at[h, e], rb.at[h, e]

        def step(i, carry):
            i = 15 - i
            zz, yy = flip2(z, lax.rem(i, 4)), flip2(y, i // 4)
            block = (zz * 4 + yy) * 8 + core * 4
            for mask in (2, 1, 3, 0):
                xx = flip(x, mask)
                to = {"seq": zz * 4 + yy, "ch": xx * 2 + core}
                one = copy(source.at[block + xx], target.at[mine], sem, done, to)
                if mask:
                    one.start()
                else:

                    @pl.when(jnp.logical_or(i > 0, k != core))
                    def _():
                        one.start()

            return carry

        lax.fori_loop(0, 16, step, 0)

    def keep(h, e):
        gathered[h, e, mine] = send[h, e, s * 8 + k * 4 + x]

    ws, wr = w_sems

    def pair(method, u, *m):
        method(u, *m)
        method(u + 1, *m)

    pair(A.F, 0)
    pair(A.S, 0, 0)
    for i in range(2):
        loads[4 + i].wait()
        turn(raw2.at[i], 0, 16)
        pack(spec.at[i])
        A.F(2 + i)
    pair(A.F, 4)
    pair(A.S, 0, 1)
    pair(A.S, 0, 3)
    pair(A.S, 2, 0)
    for i in (6, 7, 8, 9):
        loads[i].wait()
    build()
    wmine[...] = dot(order[...], w[...]).astype(BF16).reshape(2, 64, 1024)
    peers(lambda t: copy(wmine, wfull.at[:, c], ws, wr, {"seq": s, "ch": t}).start())
    wfull[:, c] = wmine[...]
    pair(A.S, 0, 2)
    pair(A.S, 4, 0)
    pair(A.S, 2, 1)
    pair(A.S, 2, 3)
    pair(A.S, 2, 2)
    pair(A.S, 4, 1)
    A.done(0)
    forward(0, 0)
    pair(A.S, 4, 3)
    A.done(1)
    peers(
        lambda t: pl.semaphore_signal(
            met, 1, device_id={"seq": s, "ch": t}, device_id_type=MESH
        )
    )
    forward(0, 2)
    pair(A.S, 4, 2)
    forward(1, 0)
    forward(1, 2)
    A.done(2)
    A.done(3)
    inverse(0, 0)
    inverse(0, 2)
    place(0)
    pl.semaphore_wait(met, 7)
    scatter_to(0, 0, 0)
    A.done(4)
    A.done(5)
    scatter_to(1, 0, 0)
    inverse(1, 0)
    inverse(1, 2)
    place(1)
    scatter_to(0, 1, 0)
    scatter_to(0, 0, 1)
    scatter_to(0, 1, 1)
    scatter_to(1, 1, 0)
    scatter_to(1, 0, 1)
    scatter_to(1, 1, 1)
    for e in range(2):
        keep(0, e)
        keep(1, e)
    recv(wfull.at[:, pl.ds(0, 7)], wr)

    ds, dr = d_sems

    def arrange(h, e):
        recv(gathered.at[h, e, pl.ds(0, 127)], rb.at[h, e])
        for i in range(4):
            value = lax.dot_general(
                gathered[h, e, 32 * i : 32 * i + 32].reshape(256, 128),
                regroup[...],
                (((0,), (0,)), ((), ())),
                preferred_element_type=F32,
            ).astype(BF16)
            rows[:128, i * 128 : (i + 1) * 128] = value[:, :128]
            rows[128:, i * 128 : (i + 1) * 128] = value[:, 128:]

    def begin(e):
        arrange(0, e)
        total[...] = dot(rows[...], wfull[0].reshape(512, 1024))

    def finish(e):
        arrange(1, e)
        for mask in (2, 1, 3, 0):
            xx = flip(x, mask)
            columns = pl.ds(pl.multiple_of(xx * 256, 256), 256)
            value = dot(rows[...], wfull[1, :, :, columns].reshape(512, 256))
            value = (total[:, columns] + value).astype(BF16)
            for core in range(2):
                part = value[:, core * 128 : (core + 1) * 128]
                prod[e, xx * 2 + core] = part.reshape(2, 128, 128)
            for core in (k, other):
                if mask or core is other:
                    to = {"seq": s, "ch": xx * 2 + core}
                    part = prod.at[e, xx * 2 + core]
                    copy(part, out.at[c, :, e], ds.at[e], dr.at[e], to).start()
        out[c, :, e] = prod[e, c]

    begin(0)
    finish(0)
    begin(1)
    finish(1)
    for e in range(2):
        recv(prod.at[e, pl.ds(0, 7)], dr.at[e])

    for u in range(6):
        A.drain(u)
    for e in range(2):
        for h in range(2):
            sent(send.at[h, e, pl.ds(0, 127)], sb.at[h, e])
        sent(prod.at[e, pl.ds(0, 7)], ds.at[e])
    sent(wfull.at[:, pl.ds(0, 7)], ws)


def per_device(signal, spectrum, channel_mode, skip_gain, out_weight):
    unit = (4, 16, 256)
    dma = pltpu.SemaphoreType.DMA
    constant = table()
    vmem = pl.BlockSpec(memory_space=pltpu.VMEM)
    hbm = pl.BlockSpec(memory_space=pltpu.HBM)
    fixed = [
        pltpu.with_memory_space_constraint(t, pltpu.HBM)
        for t in (out_weight, channel_mode, skip_gain)
    ]
    result = pl.pallas_call(
        kernel,
        out_shape=jax.ShapeDtypeStruct((8, 2, 2, 128, 128), BF16),
        in_specs=[hbm] * 6,
        out_specs=vmem,
        scratch_shapes=[
            pltpu.VMEM((16, 256, 128), F32),
            pltpu.VMEM((2, 16, 256, 128), F32),
            pltpu.VMEM((2, 128 * PITCH, 128), F32),
            pltpu.VMEM((4, 4, 2) + unit, BF16),
            pltpu.VMEM((2, 4, 4, 2) + unit, BF16),
            pltpu.VMEM((4, 256, 256), F32),
            pltpu.VMEM((128, 1024), BF16),
            pltpu.SMEM((128,), jnp.int32),
            pltpu.SMEM((128,), F32),
            pltpu.VMEM((512, 256), BF16),
            pltpu.VMEM((512, 512), BF16),
            pltpu.VMEM((512, 512), BF16),
            pltpu.VMEM((256, 512), BF16),
            pltpu.VMEM((256, 256), BF16),
            pltpu.VMEM((256, 256), BF16),
            pltpu.VMEM((128, 128), BF16),
            pltpu.VMEM((6, 3, 4) + unit, BF16),
            pltpu.VMEM((6, 4, 4) + unit, BF16),
            pltpu.VMEM((8, 256, 512), F32),
            pltpu.VMEM((4, 4, 4, 16, 256), BF16),
            pltpu.VMEM((2, 2, 128, 8, 128), BF16),
            pltpu.VMEM((2, 2, 128, 8, 128), BF16),
            pltpu.VMEM((256, 512), BF16),
            pltpu.VMEM((256, 1024), F32),
            pltpu.VMEM((2, 64, 1024), BF16),
            pltpu.VMEM((2, 8, 64, 1024), BF16),
            pltpu.VMEM((2, 8, 2, 128, 128), BF16),
            dma((10,)),
            (dma((6,)), dma((6,)), dma((6,)), dma((6, 3))),
            (dma((2, 2)), dma((2, 2))),
            (dma, dma),
            (dma((2,)), dma((2,))),
            pltpu.SemaphoreType.REGULAR,
        ],
        compiler_params=pltpu.CompilerParams(
            collective_id=0, has_side_effects=True, vmem_limit_bytes=52 << 20
        ),
        name="hyena",
    )(
        signal.reshape(16, 256, 128), spectrum, *fixed, constant
    )
    return result.astype(F32).reshape(1, 4096, 128)


def solution(mesh):
    in_specs = (
        P(None, "seq", "ch"), P(None, "seq", None, "ch"), P("ch"), P("ch"), P("ch", None)
    )
    return jax.shard_map(
        per_device, mesh=mesh, in_specs=in_specs, out_specs=P(None, "seq", "ch"), check_vma=False
    )
```

```python
import math

import jax
import jax.numpy as jnp
import numpy as np
from jax import lax
from jax.experimental import pallas as pl
from jax.experimental.pallas import tpu as pltpu
from jax.sharding import PartitionSpec as P

ROWS = 256
COLUMNS = 256
LENGTH = 65536
BF16 = jnp.bfloat16
F32 = jnp.float32
MESH = pl.DeviceIdType.MESH


PITCH = 24


def table():
    counter = np.arange(256)
    product = counter[:, None] * counter[None, :]
    angle = product % 256 * (2.0 * math.pi / 256)
    twist = product * (2.0 * math.pi / LENGTH)
    parts = [np.cos(angle), np.sin(angle), np.cos(twist), np.sin(twist)]
    return jnp.asarray(np.stack(parts), F32)


def flip(v, mask):
    if mask == 0:
        return v
    if mask == 1:
        return v + 1 - 2 * lax.rem(v, 2)
    if mask == 2:
        return lax.rem(v + 2, 4)
    return 3 - v


def dot(a, b):
    return jnp.dot(a, b, preferred_element_type=F32)


def flip2(v, step):
    return lax.rem(v + jnp.where(step == 3, 2, jnp.where(step == 2, 3, step)), 4)


def kernel(
    signal, spectrum, w_hbm, mode_hbm, gain_hbm, table_hbm,
    out,
    raw, raw2, turned, sig, spec, twist, w, mode, gain,
    first, second, third, last, scatter, regroup, order,
    buf, final, spectral, mixed, hid, send, gathered, rows, total, wmine, wfull, prod,
    h_sems, a_sems, b_sems, w_sems, d_sems, met,
):
    s = lax.axis_index("seq")
    c = lax.axis_index("ch")
    z, y, x, k = s // 4, lax.rem(s, 4), c // 2, lax.rem(c, 2)
    other = 1 - k

    def zdev(mask):
        return {"seq": flip(z, mask) * 4 + y, "ch": c}

    def ydev(mask):
        return {"seq": z * 4 + flip(y, mask), "ch": c}

    def xdev(mask):
        return {"seq": s, "ch": flip(x, mask) * 2 + k}

    partner = {"seq": s, "ch": x * 2 + other}

    def copy(a, b, ss, rs, dev):
        return pltpu.make_async_remote_copy(a, b, ss, rs, device_id=dev, device_id_type=MESH)

    def recv(ref, sem):
        copy(ref, ref, sem, sem, partner).wait_recv()

    def sent(ref, sem):
        copy(ref, ref, sem, sem, partner).wait_send()

    def peers(fn):
        for mask in (2, 1, 3, 0):
            for core in (k, other):
                if mask or core is other:
                    fn(flip(x, mask) * 2 + core)

    loads = [
        pltpu.make_async_copy(signal.at[pl.ds(4 * i, 4)], raw.at[pl.ds(4 * i, 4)], h_sems.at[i])
        for i in range(4)
    ]
    loads += [
        pltpu.make_async_copy(spectrum.at[i], raw2.at[i], h_sems.at[4 + i]) for i in range(2)
    ]
    small = ((table_hbm, twist), (w_hbm, w), (mode_hbm, mode), (gain_hbm, gain))
    for i, (a, b) in enumerate(small):
        loads.append(pltpu.make_async_copy(a, b, h_sems.at[6 + i]))
    for load in loads:
        load.start()

    barrier = pltpu.get_barrier_semaphore()

    def greet(dev):
        pl.semaphore_signal(barrier, 1, device_id=dev, device_id_type=MESH)

    for mask in (1, 2, 3):
        greet(zdev(mask))
        greet(ydev(mask))
    peers(lambda t: greet({"seq": s, "ch": t}))

    def turn(source, lo, n):
        def step(a, carry):
            value = source[a].T
            turned.at[0][pl.ds(a, 128, stride=PITCH), :] = value[:, :128]
            turned.at[1][pl.ds(a, 128, stride=PITCH), :] = value[:, 128:]
            return carry

        lax.fori_loop(lo, lo + n, step, 0, unroll=4)

    def pack(target):
        def step(t, carry):
            for h in range(2):
                for m in range(4):
                    at = pl.ds(pl.multiple_of((t * 8 + h * 4 + m) * PITCH, 8), 16)
                    value = jnp.concatenate([turned[0, at, :], turned[1, at, :]], 1)
                    target[t // 4, lax.rem(t, 4), h, m] = value.astype(BF16)
            return carry

        lax.fori_loop(0, 16, step, 0)

    for i in range(4):
        loads[i].wait()
        turn(raw, 4 * i, 4)
    pack(sig)
    pl.semaphore_wait(barrier, 13)

    class Plane:
        def __init__(self, grab, buf, final, sems):
            self.grab, self.buf, self.final = grab, buf, final
            self.s1, self.s2, self.rfin, self.rbuf = sems

        def dev(self, u, leg, mask):
            return zdev(mask) if u % 2 == leg else ydev(mask)

        def F(self, u):
            for mask in (2, 1, 3):
                if u % 2 == 0:
                    row = self.grab(u, flip(z, mask), slice(None))
                else:
                    row = self.grab(u, slice(None), flip(y, mask))
                to, sem = self.buf.at[u, mask - 1], self.rbuf.at[u, mask - 1]
                copy(row, to, self.s1.at[u], sem, self.dev(u, 0, mask)).start()

        def S(self, u, m1):
            if m1:
                recv(self.buf.at[u, m1 - 1], self.rbuf.at[u, m1 - 1])
            for mask in (2, 1, 3, 0):
                other = flip(y if u % 2 == 0 else z, mask)
                if m1:
                    part = self.buf.at[u, m1 - 1, other]
                else:
                    part = self.grab(u, z, other) if u % 2 == 0 else self.grab(u, other, y)
                if u % 2 == 0:
                    slot = self.final.at[u, flip(z, m1), y]
                else:
                    slot = self.final.at[u, z, flip(y, m1)]
                if mask:
                    to = self.dev(u, 1, mask)
                    copy(part, slot, self.s2.at[u], self.rfin.at[u], to).start()
                else:
                    slot[...] = part[...]

        def done(self, u):
            recv(self.final.at[u, pl.ds(0, 3)], self.rfin.at[u])

        def drain(self, u):
            sent(self.final.at[u, pl.ds(0, 3)], self.s1.at[u])
            sent(self.final.at[u, pl.ds(0, 3)], self.s2.at[u])

    def grab_inputs(u, zi, yi):
        if u < 2:
            return sig.at[zi, yi, u]
        return spec.at[u % 2, zi, yi, u // 2 - 1]

    A = Plane(grab_inputs, buf, final, a_sems)

    def twists(ch, columns=slice(None)):
        on = mode[s * 8 + ch] == 1
        tc = jnp.where(on, twist[2, :, columns], 1.0)
        return tc, jnp.where(on, twist[3, :, columns], 0.0)

    def forward(h, lo):
        def step(m, carry):
            image = final[h, :, :, m].reshape(256, 256)
            value = dot(first[...], image)
            re, im = value[:256], value[256:]
            tc, ts = twists(4 * h + m)
            pair = jnp.concatenate([re * tc + im * ts, im * tc - re * ts], 1).astype(BF16)
            spectral[4 * h + m] = dot(pair, second[...])
            return carry

        lax.fori_loop(lo, lo + 2, step, 0, unroll=True)

    def inverse(h, e):
        columns = slice(e * 128, e * 128 + 128)

        def step(j, carry):
            parts = []
            for m in (2 * j, 2 * j + 1):
                if e == 0:
                    value = spectral[4 * h + m]
                    re, im = value[:, :256], value[:, 256:]
                    fr = final[2 + 2 * h, :, :, m].reshape(256, 256).astype(F32)
                    fi = final[3 + 2 * h, :, :, m].reshape(256, 256).astype(F32)
                    pair = jnp.concatenate([re * fr - im * fi, re * fi + im * fr], 1).astype(BF16)
                    mixed[m] = pair
                else:
                    pair = mixed[m]
                value = dot(pair, third[e])
                re, im = value[:, :128], value[:, 128:]
                tc, ts = twists(4 * h + m, columns)
                pair = jnp.concatenate([re * tc - im * ts, re * ts + im * tc], 0)
                parts.append(pair.astype(BF16))
            value = dot(last[...], jnp.concatenate(parts, 1))
            for n in range(2):
                m = 2 * j + n
                image = final[h, :, :, m, :, columns].reshape(256, 128).astype(F32)
                part = value[:, n * 128 : (n + 1) * 128] + gain[s * 8 + 4 * h + m] * image
                hid[e, m] = part.astype(BF16).reshape(4, 4, 16, 128)
            return carry

        lax.fori_loop(0, 2, step, 0, unroll=True)

    def build():
        cos, sin = twist[0], twist[1]
        first[:256], first[256:] = cos.astype(BF16), (-sin).astype(BF16)
        second[:256, :256] = second[256:, 256:] = cos.astype(BF16)
        second[:256, 256:] = (-sin).astype(BF16)
        second[256:, :256] = sin.astype(BF16)
        for e in range(2):
            part = slice(e * 128, e * 128 + 128)
            third[e, :256, :128] = third[e, 256:, 128:] = cos[:, part].astype(BF16)
            third[e, 256:, :128] = (-sin[:, part]).astype(BF16)
            third[e, :256, 128:] = sin[:, part].astype(BF16)
        last[:, :256] = (cos / LENGTH).astype(BF16)
        last[:, 256:] = (-sin / LENGTH).astype(BF16)
        i = lax.broadcasted_iota(jnp.int32, (256, 256), 0)
        j = lax.broadcasted_iota(jnp.int32, (256, 256), 1)
        m, t, at = j >> 6, (j >> 4) & 3, j & 15
        row = t * 64 + ((at >> 1) & 1) * 32 + (at >> 2) * 8 + (at & 1) * 4 + m
        scatter[...] = jnp.where(i == row, 1.0, 0.0).astype(BF16)
        column = ((i >> 2) & 1) * 128 + (i >> 7) * 64 + ((i >> 3) & 15) * 4 + (i & 3)
        regroup[...] = jnp.where(j == column, 1.0, 0.0).astype(BF16)
        i, j = i[:128, :128], j[:128, :128]
        row = ((j >> 2) & 1) * 64 + (j >> 3) * 4 + (j & 3)
        order[...] = jnp.where(i == row, 1.0, 0.0).astype(BF16)

    def place(h, e):
        for t in (0, 2):
            blocks = [hid[e, :, t + n].reshape(256, 128) for n in range(2)]
            value = dot(scatter[...], jnp.concatenate(blocks, 1)).astype(BF16)
            for n in range(2):
                part = value[:, n * 128 : (n + 1) * 128]
                send[h, e, (t + n) * 32 : (t + n + 1) * 32] = part.reshape(32, 8, 128)

    sb, rb = b_sems
    mine = c * 16 + s

    def scatter_to(core, h, e):
        source, target = send.at[h, e], gathered.at[h, e]
        sem, done = sb.at[h, e], rb.at[h, e]

        def step(i, carry):
            i = 15 - i
            zz, yy = flip2(z, lax.rem(i, 4)), flip2(y, i // 4)
            block = (zz * 4 + yy) * 8 + core * 4
            for mask in (2, 1, 3, 0):
                xx = flip(x, mask)
                to = {"seq": zz * 4 + yy, "ch": xx * 2 + core}
                one = copy(source.at[block + xx], target.at[mine], sem, done, to)
                if mask:
                    one.start()
                else:

                    @pl.when(jnp.logical_or(i > 0, k != core))
                    def _():
                        one.start()

            return carry

        lax.fori_loop(0, 16, step, 0)

    def keep(h, e):
        gathered[h, e, mine] = send[h, e, s * 8 + k * 4 + x]

    ws, wr = w_sems

    def pair(method, u, *m):
        method(u, *m)
        method(u + 1, *m)

    pair(A.F, 0)
    pair(A.S, 0, 0)
    for i in range(2):
        loads[4 + i].wait()
        turn(raw2.at[i], 0, 16)
        pack(spec.at[i])
        A.F(2 + i)
    pair(A.F, 4)
    pair(A.S, 0, 1)
    pair(A.S, 0, 3)
    pair(A.S, 2, 0)
    for i in (6, 7, 8, 9):
        loads[i].wait()
    build()
    wmine[...] = dot(order[...], w[...]).astype(BF16).reshape(2, 64, 1024)
    peers(lambda t: copy(wmine, wfull.at[:, c], ws, wr, {"seq": s, "ch": t}).start())
    wfull[:, c] = wmine[...]
    pair(A.S, 0, 2)
    pair(A.S, 4, 0)
    pair(A.S, 2, 1)
    pair(A.S, 2, 3)
    pair(A.S, 2, 2)
    pair(A.S, 4, 1)
    A.done(0)
    forward(0, 0)
    pair(A.S, 4, 3)
    A.done(1)
    peers(
        lambda t: pl.semaphore_signal(
            met, 1, device_id={"seq": s, "ch": t}, device_id_type=MESH
        )
    )
    forward(0, 2)
    pair(A.S, 4, 2)
    forward(1, 0)
    forward(1, 2)
    A.done(2)
    A.done(3)
    inverse(0, 0)
    place(0, 0)
    pl.semaphore_wait(met, 7)
    scatter_to(0, 0, 0)
    inverse(0, 1)
    place(0, 1)
    A.done(4)
    A.done(5)
    scatter_to(1, 0, 0)
    inverse(1, 0)
    place(1, 0)
    scatter_to(0, 1, 0)
    scatter_to(0, 0, 1)
    inverse(1, 1)
    place(1, 1)
    scatter_to(0, 1, 1)
    scatter_to(1, 1, 0)
    scatter_to(1, 0, 1)
    scatter_to(1, 1, 1)
    for e in range(2):
        keep(0, e)
        keep(1, e)
    recv(wfull.at[:, pl.ds(0, 7)], wr)

    ds, dr = d_sems

    def arrange(h, e):
        recv(gathered.at[h, e, pl.ds(0, 127)], rb.at[h, e])
        for i in range(4):
            value = lax.dot_general(
                gathered[h, e, 32 * i : 32 * i + 32].reshape(256, 128),
                regroup[...],
                (((0,), (0,)), ((), ())),
                preferred_element_type=F32,
            ).astype(BF16)
            rows[:128, i * 128 : (i + 1) * 128] = value[:, :128]
            rows[128:, i * 128 : (i + 1) * 128] = value[:, 128:]

    def begin(e):
        arrange(0, e)
        total[...] = dot(rows[...], wfull[0].reshape(512, 1024))

    def finish(e):
        arrange(1, e)
        for mask in (2, 1, 3, 0):
            xx = flip(x, mask)
            columns = pl.ds(pl.multiple_of(xx * 256, 256), 256)
            value = dot(rows[...], wfull[1, :, :, columns].reshape(512, 256))
            value = (total[:, columns] + value).astype(BF16)
            for core in range(2):
                part = value[:, core * 128 : (core + 1) * 128]
                prod[e, xx * 2 + core] = part.reshape(2, 128, 128)
            for core in (k, other):
                if mask or core is other:
                    to = {"seq": s, "ch": xx * 2 + core}
                    part = prod.at[e, xx * 2 + core]
                    copy(part, out.at[c, :, e], ds.at[e], dr.at[e], to).start()
        out[c, :, e] = prod[e, c]

    begin(0)
    finish(0)
    begin(1)
    finish(1)
    for e in range(2):
        recv(prod.at[e, pl.ds(0, 7)], dr.at[e])

    for u in range(6):
        A.drain(u)
    for e in range(2):
        for h in range(2):
            sent(send.at[h, e, pl.ds(0, 127)], sb.at[h, e])
        sent(prod.at[e, pl.ds(0, 7)], ds.at[e])
    sent(wfull.at[:, pl.ds(0, 7)], ws)


def per_device(signal, spectrum, channel_mode, skip_gain, out_weight):
    unit = (4, 16, 256)
    dma = pltpu.SemaphoreType.DMA
    constant = table()
    vmem = pl.BlockSpec(memory_space=pltpu.VMEM)
    hbm = pl.BlockSpec(memory_space=pltpu.HBM)
    fixed = [
        pltpu.with_memory_space_constraint(t, pltpu.HBM)
        for t in (out_weight, channel_mode, skip_gain)
    ]
    result = pl.pallas_call(
        kernel,
        out_shape=jax.ShapeDtypeStruct((8, 2, 2, 128, 128), BF16),
        in_specs=[hbm] * 6,
        out_specs=vmem,
        scratch_shapes=[
            pltpu.VMEM((16, 256, 128), F32),
            pltpu.VMEM((2, 16, 256, 128), F32),
            pltpu.VMEM((2, 128 * PITCH, 128), F32),
            pltpu.VMEM((4, 4, 2) + unit, BF16),
            pltpu.VMEM((2, 4, 4, 2) + unit, BF16),
            pltpu.VMEM((4, 256, 256), F32),
            pltpu.VMEM((128, 1024), BF16),
            pltpu.SMEM((128,), jnp.int32),
            pltpu.SMEM((128,), F32),
            pltpu.VMEM((512, 256), BF16),
            pltpu.VMEM((512, 512), BF16),
            pltpu.VMEM((2, 512, 256), BF16),
            pltpu.VMEM((256, 512), BF16),
            pltpu.VMEM((256, 256), BF16),
            pltpu.VMEM((256, 256), BF16),
            pltpu.VMEM((128, 128), BF16),
            pltpu.VMEM((6, 3, 4) + unit, BF16),
            pltpu.VMEM((6, 4, 4) + unit, BF16),
            pltpu.VMEM((8, 256, 512), F32),
            pltpu.VMEM((4, 256, 512), BF16),
            pltpu.VMEM((2, 4, 4, 4, 16, 128), BF16),
            pltpu.VMEM((2, 2, 128, 8, 128), BF16),
            pltpu.VMEM((2, 2, 128, 8, 128), BF16),
            pltpu.VMEM((256, 512), BF16),
            pltpu.VMEM((256, 1024), F32),
            pltpu.VMEM((2, 64, 1024), BF16),
            pltpu.VMEM((2, 8, 64, 1024), BF16),
            pltpu.VMEM((2, 8, 2, 128, 128), BF16),
            dma((10,)),
            (dma((6,)), dma((6,)), dma((6,)), dma((6, 3))),
            (dma((2, 2)), dma((2, 2))),
            (dma, dma),
            (dma((2,)), dma((2,))),
            pltpu.SemaphoreType.REGULAR,
        ],
        compiler_params=pltpu.CompilerParams(
            collective_id=0, has_side_effects=True, vmem_limit_bytes=52 << 20
        ),
        name="hyena",
    )(
        signal.reshape(16, 256, 128), spectrum, *fixed, constant
    )
    return result.astype(F32).reshape(1, 4096, 128)


def solution(mesh):
    in_specs = (
        P(None, "seq", "ch"), P(None, "seq", None, "ch"), P("ch"), P("ch"), P("ch", None)
    )
    return jax.shard_map(
        per_device, mesh=mesh, in_specs=in_specs, out_specs=P(None, "seq", "ch"), check_vma=False
    )
```

```python
import math

import jax
import jax.numpy as jnp
import numpy as np
from jax import lax
from jax.experimental import pallas as pl
from jax.experimental.pallas import tpu as pltpu
from jax.sharding import PartitionSpec as P

ROWS = 256
COLUMNS = 256
LENGTH = 65536
BF16 = jnp.bfloat16
F32 = jnp.float32
MESH = pl.DeviceIdType.MESH


PITCH = 24


def table():
    counter = np.arange(256)
    product = counter[:, None] * counter[None, :]
    angle = product % 256 * (2.0 * math.pi / 256)
    twist = product * (2.0 * math.pi / LENGTH)
    parts = [np.cos(angle), np.sin(angle), np.cos(twist), np.sin(twist)]
    return jnp.asarray(np.stack(parts), F32)


def flip(v, mask):
    if mask == 0:
        return v
    if mask == 1:
        return v + 1 - 2 * lax.rem(v, 2)
    if mask == 2:
        return lax.rem(v + 2, 4)
    return 3 - v


def dot(a, b):
    return jnp.dot(a, b, preferred_element_type=F32)


def flip2(v, step):
    return lax.rem(v + jnp.where(step == 3, 2, jnp.where(step == 2, 3, step)), 4)


def kernel(
    signal, spectrum, w_hbm, mode_hbm, gain_hbm, table_hbm,
    out,
    raw, raw2, turned, sig, spec, twist, w, mode, gain,
    first, second, third, last, scatter, regroup, order,
    buf, final, spectral, mixed, hid, send, gathered, rows, total, wmine, wfull, prod,
    h_sems, a_sems, b_sems, w_sems, d_sems, met,
):
    s = lax.axis_index("seq")
    c = lax.axis_index("ch")
    z, y, x, k = s // 4, lax.rem(s, 4), c // 2, lax.rem(c, 2)
    other = 1 - k

    def zdev(mask):
        return {"seq": flip(z, mask) * 4 + y, "ch": c}

    def ydev(mask):
        return {"seq": z * 4 + flip(y, mask), "ch": c}

    def xdev(mask):
        return {"seq": s, "ch": flip(x, mask) * 2 + k}

    partner = {"seq": s, "ch": x * 2 + other}

    def copy(a, b, ss, rs, dev):
        return pltpu.make_async_remote_copy(a, b, ss, rs, device_id=dev, device_id_type=MESH)

    def recv(ref, sem):
        copy(ref, ref, sem, sem, partner).wait_recv()

    def sent(ref, sem):
        copy(ref, ref, sem, sem, partner).wait_send()

    def peers(fn):
        for mask in (2, 1, 3, 0):
            for core in (k, other):
                if mask or core is other:
                    fn(flip(x, mask) * 2 + core)

    loads = [
        pltpu.make_async_copy(signal.at[pl.ds(4 * i, 4)], raw.at[pl.ds(4 * i, 4)], h_sems.at[i])
        for i in range(4)
    ]
    loads += [
        pltpu.make_async_copy(spectrum.at[i], raw2.at[i], h_sems.at[4 + i]) for i in range(2)
    ]
    small = ((table_hbm, twist), (w_hbm, w), (mode_hbm, mode), (gain_hbm, gain))
    for i, (a, b) in enumerate(small):
        loads.append(pltpu.make_async_copy(a, b, h_sems.at[6 + i]))
    for load in loads:
        load.start()

    barrier = pltpu.get_barrier_semaphore()

    def greet(dev):
        pl.semaphore_signal(barrier, 1, device_id=dev, device_id_type=MESH)

    for mask in (1, 2, 3):
        greet(zdev(mask))
        greet(ydev(mask))
    peers(lambda t: greet({"seq": s, "ch": t}))

    def turn(source, lo, n):
        def step(a, carry):
            value = source[a].T
            turned.at[0][pl.ds(a, 128, stride=PITCH), :] = value[:, :128]
            turned.at[1][pl.ds(a, 128, stride=PITCH), :] = value[:, 128:]
            return carry

        lax.fori_loop(lo, lo + n, step, 0, unroll=4)

    def pack(target):
        def step(t, carry):
            for h in range(2):
                for m in range(4):
                    at = pl.ds(pl.multiple_of((t * 8 + h * 4 + m) * PITCH, 8), 16)
                    value = jnp.concatenate([turned[0, at, :], turned[1, at, :]], 1)
                    target[t // 4, lax.rem(t, 4), h, m] = value.astype(BF16)
            return carry

        lax.fori_loop(0, 16, step, 0)

    for i in range(4):
        loads[i].wait()
        turn(raw, 4 * i, 4)
    pack(sig)
    pl.semaphore_wait(barrier, 13)

    class Plane:
        def __init__(self, grab, buf, final, sems):
            self.grab, self.buf, self.final = grab, buf, final
            self.s1, self.s2, self.rfin, self.rbuf = sems

        def dev(self, u, leg, mask):
            return zdev(mask) if u % 2 == leg else ydev(mask)

        def F(self, u):
            for mask in (2, 1, 3):
                if u % 2 == 0:
                    row = self.grab(u, flip(z, mask), slice(None))
                else:
                    row = self.grab(u, slice(None), flip(y, mask))
                to, sem = self.buf.at[u, mask - 1], self.rbuf.at[u, mask - 1]
                copy(row, to, self.s1.at[u], sem, self.dev(u, 0, mask)).start()

        def S(self, u, m1):
            if m1:
                recv(self.buf.at[u, m1 - 1], self.rbuf.at[u, m1 - 1])
            for mask in (2, 1, 3, 0):
                other = flip(y if u % 2 == 0 else z, mask)
                if m1:
                    part = self.buf.at[u, m1 - 1, other]
                else:
                    part = self.grab(u, z, other) if u % 2 == 0 else self.grab(u, other, y)
                if u % 2 == 0:
                    slot = self.final.at[u, flip(z, m1), y]
                else:
                    slot = self.final.at[u, z, flip(y, m1)]
                if mask:
                    to = self.dev(u, 1, mask)
                    copy(part, slot, self.s2.at[u], self.rfin.at[u], to).start()
                else:
                    slot[...] = part[...]

        def done(self, u):
            recv(self.final.at[u, pl.ds(0, 3)], self.rfin.at[u])

        def drain(self, u):
            sent(self.final.at[u, pl.ds(0, 3)], self.s1.at[u])
            sent(self.final.at[u, pl.ds(0, 3)], self.s2.at[u])

    def grab_inputs(u, zi, yi):
        if u < 2:
            return sig.at[zi, yi, u]
        return spec.at[u % 2, zi, yi, u // 2 - 1]

    A = Plane(grab_inputs, buf, final, a_sems)

    def twists(ch, columns=slice(None)):
        on = mode[s * 8 + ch] == 1
        tc = jnp.where(on, twist[2, :, columns], 1.0)
        return tc, jnp.where(on, twist[3, :, columns], 0.0)

    def forward(h, lo):
        def step(m, carry):
            image = final[h, :, :, m].reshape(256, 256)
            value = dot(first[...], image)
            re, im = value[:256], value[256:]
            tc, ts = twists(4 * h + m)
            pair = jnp.concatenate([re * tc + im * ts, im * tc - re * ts], 1).astype(BF16)
            spectral[4 * h + m] = dot(pair, second[...])
            return carry

        lax.fori_loop(lo, lo + 2, step, 0, unroll=True)

    def inverse(h, e):
        columns = slice(e * 128, e * 128 + 128)

        def step(j, carry):
            parts = []
            for m in (2 * j, 2 * j + 1):
                if e == 0:
                    value = spectral[4 * h + m]
                    re, im = value[:, :256], value[:, 256:]
                    fr = final[2 + 2 * h, :, :, m].reshape(256, 256).astype(F32)
                    fi = final[3 + 2 * h, :, :, m].reshape(256, 256).astype(F32)
                    pair = jnp.concatenate([re * fr - im * fi, re * fi + im * fr], 1).astype(BF16)
                    mixed[m] = pair
                else:
                    pair = mixed[m]
                value = dot(pair, third[e])
                re, im = value[:, :128], value[:, 128:]
                tc, ts = twists(4 * h + m, columns)
                pair = jnp.concatenate([re * tc - im * ts, re * ts + im * tc], 0)
                parts.append(pair.astype(BF16))
            value = dot(last[...], jnp.concatenate(parts, 1))
            for n in range(2):
                m = 2 * j + n
                image = final[h, :, :, m, :, columns].reshape(256, 128).astype(F32)
                part = value[:, n * 128 : (n + 1) * 128] + gain[s * 8 + 4 * h + m] * image
                hid[e, m] = part.astype(BF16).reshape(4, 4, 16, 128)
            return carry

        lax.fori_loop(0, 2, step, 0, unroll=True)

    def build():
        cos, sin = twist[0], twist[1]
        first[:256], first[256:] = cos.astype(BF16), (-sin).astype(BF16)
        second[:256, :256] = second[256:, 256:] = cos.astype(BF16)
        second[:256, 256:] = (-sin).astype(BF16)
        second[256:, :256] = sin.astype(BF16)
        for e in range(2):
            part = slice(e * 128, e * 128 + 128)
            third[e, :256, :128] = third[e, 256:, 128:] = cos[:, part].astype(BF16)
            third[e, 256:, :128] = (-sin[:, part]).astype(BF16)
            third[e, :256, 128:] = sin[:, part].astype(BF16)
        last[:, :256] = (cos / LENGTH).astype(BF16)
        last[:, 256:] = (-sin / LENGTH).astype(BF16)
        i = lax.broadcasted_iota(jnp.int32, (256, 256), 0)
        j = lax.broadcasted_iota(jnp.int32, (256, 256), 1)
        m, t, at = j >> 6, (j >> 4) & 3, j & 15
        row = t * 64 + ((at >> 1) & 1) * 32 + (at >> 2) * 8 + (at & 1) * 4 + m
        scatter[...] = jnp.where(i == row, 1.0, 0.0).astype(BF16)
        column = ((i >> 2) & 1) * 128 + (i >> 7) * 64 + ((i >> 3) & 15) * 4 + (i & 3)
        regroup[...] = jnp.where(j == column, 1.0, 0.0).astype(BF16)
        i, j = i[:128, :128], j[:128, :128]
        row = ((j >> 2) & 1) * 64 + (j >> 3) * 4 + (j & 3)
        order[...] = jnp.where(i == row, 1.0, 0.0).astype(BF16)

    def place(h, e):
        for t in (0, 2):
            blocks = [hid[e, :, t + n].reshape(256, 128) for n in range(2)]
            value = dot(scatter[...], jnp.concatenate(blocks, 1)).astype(BF16)
            for n in range(2):
                part = value[:, n * 128 : (n + 1) * 128]
                send[h, e, (t + n) * 32 : (t + n + 1) * 32] = part.reshape(32, 8, 128)

    sb, rb = b_sems
    mine = c * 16 + s

    def scatter_to(core, h, e):
        source, target = send.at[h, e], gathered.at[h, e]
        sem, done = sb.at[h, e], rb.at[h, e]

        def step(i, carry):
            i = 15 - i
            zz, yy = flip2(z, lax.rem(i, 4)), flip2(y, i // 4)
            block = (zz * 4 + yy) * 8 + core * 4
            for mask in (2, 1, 3, 0):
                xx = flip(x, mask)
                to = {"seq": zz * 4 + yy, "ch": xx * 2 + core}
                one = copy(source.at[block + xx], target.at[mine], sem, done, to)
                if mask:
                    one.start()
                else:

                    @pl.when(jnp.logical_or(i > 0, k != core))
                    def _():
                        one.start()

            return carry

        lax.fori_loop(0, 16, step, 0)

    def keep(h, e):
        gathered[h, e, mine] = send[h, e, s * 8 + k * 4 + x]

    ws, wr = w_sems

    def pair(method, u, *m):
        method(u, *m)
        method(u + 1, *m)

    pair(A.F, 0)
    pair(A.S, 0, 0)
    for i in range(2):
        loads[4 + i].wait()
        turn(raw2.at[i], 0, 16)
        pack(spec.at[i])
        A.F(2 + i)
    pair(A.F, 4)
    pair(A.S, 0, 1)
    pair(A.S, 0, 3)
    pair(A.S, 2, 0)
    for i in (6, 7, 8, 9):
        loads[i].wait()
    build()
    wmine[...] = dot(order[...], w[...]).astype(BF16).reshape(2, 64, 1024)
    peers(lambda t: copy(wmine, wfull.at[:, c], ws, wr, {"seq": s, "ch": t}).start())
    wfull[:, c] = wmine[...]
    pair(A.S, 0, 2)
    pair(A.S, 4, 0)
    pair(A.S, 2, 1)
    pair(A.S, 2, 3)
    pair(A.S, 2, 2)
    pair(A.S, 4, 1)
    A.done(0)
    forward(0, 0)
    pair(A.S, 4, 3)
    A.done(1)
    peers(
        lambda t: pl.semaphore_signal(
            met, 1, device_id={"seq": s, "ch": t}, device_id_type=MESH
        )
    )
    forward(0, 2)
    pair(A.S, 4, 2)
    forward(1, 0)
    forward(1, 2)
    A.done(2)
    A.done(3)
    inverse(0, 0)
    place(0, 0)
    pl.semaphore_wait(met, 7)
    scatter_to(0, 0, 0)
    inverse(0, 1)
    place(0, 1)
    A.done(4)
    A.done(5)
    scatter_to(1, 0, 0)
    inverse(1, 0)
    place(1, 0)
    scatter_to(0, 1, 0)
    scatter_to(0, 0, 1)
    inverse(1, 1)
    place(1, 1)
    scatter_to(0, 1, 1)
    scatter_to(1, 1, 0)
    scatter_to(1, 0, 1)
    scatter_to(1, 1, 1)
    for e in range(2):
        keep(0, e)
        keep(1, e)
    recv(wfull.at[:, pl.ds(0, 7)], wr)

    ds, dr = d_sems

    def arrange(h, e):
        recv(gathered.at[h, e, pl.ds(0, 127)], rb.at[h, e])
        for i in range(4):
            value = lax.dot_general(
                gathered[h, e, 32 * i : 32 * i + 32].reshape(256, 128),
                regroup[...],
                (((0,), (0,)), ((), ())),
                preferred_element_type=F32,
            ).astype(BF16)
            rows[:128, i * 128 : (i + 1) * 128] = value[:, :128]
            rows[128:, i * 128 : (i + 1) * 128] = value[:, 128:]

    def begin(e):
        arrange(0, e)
        total[...] = dot(rows[...], wfull[0].reshape(512, 1024))

    def finish(e):
        arrange(1, e)
        for mask in (2, 1, 3, 0):
            xx = flip(x, mask)
            columns = pl.ds(pl.multiple_of(xx * 256, 256), 256)
            value = dot(rows[...], wfull[1, :, :, columns].reshape(512, 256))
            value = (total[:, columns] + value).astype(BF16)
            for core in range(2):
                part = value[:, core * 128 : (core + 1) * 128]
                prod[e, xx * 2 + core] = part.reshape(2, 128, 128)
            for core in (k, other):
                if mask or core is other:
                    to = {"seq": s, "ch": xx * 2 + core}
                    part = prod.at[e, xx * 2 + core]
                    copy(part, out.at[c, :, e], ds.at[e], dr.at[e], to).start()
        out[c, :, e] = prod[e, c]

    begin(0)
    finish(0)
    begin(1)
    finish(1)
    for e in range(2):
        recv(prod.at[e, pl.ds(0, 7)], dr.at[e])

    for u in range(6):
        A.drain(u)
    for e in range(2):
        for h in range(2):
            sent(send.at[h, e, pl.ds(0, 127)], sb.at[h, e])
        sent(prod.at[e, pl.ds(0, 7)], ds.at[e])
    sent(wfull.at[:, pl.ds(0, 7)], ws)


def per_device(signal, spectrum, channel_mode, skip_gain, out_weight):
    unit = (4, 16, 256)
    dma = pltpu.SemaphoreType.DMA
    constant = table()
    vmem = pl.BlockSpec(memory_space=pltpu.VMEM)
    hbm = pl.BlockSpec(memory_space=pltpu.HBM)
    fixed = [
        pltpu.with_memory_space_constraint(t, pltpu.HBM)
        for t in (out_weight, channel_mode, skip_gain)
    ]
    result = pl.pallas_call(
        kernel,
        out_shape=jax.ShapeDtypeStruct((8, 2, 2, 128, 128), BF16),
        in_specs=[hbm] * 6,
        out_specs=vmem,
        scratch_shapes=[
            pltpu.VMEM((16, 256, 128), F32),
            pltpu.VMEM((2, 16, 256, 128), F32),
            pltpu.VMEM((2, 129 * PITCH, 128), F32),
            pltpu.VMEM((4, 4, 2) + unit, BF16),
            pltpu.VMEM((2, 4, 4, 2) + unit, BF16),
            pltpu.VMEM((4, 256, 256), F32),
            pltpu.VMEM((128, 1024), BF16),
            pltpu.SMEM((128,), jnp.int32),
            pltpu.SMEM((128,), F32),
            pltpu.VMEM((512, 256), BF16),
            pltpu.VMEM((512, 512), BF16),
            pltpu.VMEM((2, 512, 256), BF16),
            pltpu.VMEM((256, 512), BF16),
            pltpu.VMEM((256, 256), BF16),
            pltpu.VMEM((256, 256), BF16),
            pltpu.VMEM((128, 128), BF16),
            pltpu.VMEM((6, 3, 4) + unit, BF16),
            pltpu.VMEM((6, 4, 4) + unit, BF16),
            pltpu.VMEM((8, 256, 512), F32),
            pltpu.VMEM((4, 256, 512), BF16),
            pltpu.VMEM((2, 4, 4, 4, 16, 128), BF16),
            pltpu.VMEM((2, 2, 128, 8, 128), BF16),
            pltpu.VMEM((2, 2, 128, 8, 128), BF16),
            pltpu.VMEM((256, 512), BF16),
            pltpu.VMEM((256, 1024), F32),
            pltpu.VMEM((2, 64, 1024), BF16),
            pltpu.VMEM((2, 8, 64, 1024), BF16),
            pltpu.VMEM((2, 8, 2, 128, 128), BF16),
            dma((10,)),
            (dma((6,)), dma((6,)), dma((6,)), dma((6, 3))),
            (dma((2, 2)), dma((2, 2))),
            (dma, dma),
            (dma((2,)), dma((2,))),
            pltpu.SemaphoreType.REGULAR,
        ],
        compiler_params=pltpu.CompilerParams(
            collective_id=0, has_side_effects=True, vmem_limit_bytes=52 << 20
        ),
        name="hyena",
    )(
        signal.reshape(16, 256, 128), spectrum, *fixed, constant
    )
    return result.astype(F32).reshape(1, 4096, 128)


def solution(mesh):
    in_specs = (
        P(None, "seq", "ch"), P(None, "seq", None, "ch"), P("ch"), P("ch"), P("ch", None)
    )
    return jax.shard_map(
        per_device, mesh=mesh, in_specs=in_specs, out_specs=P(None, "seq", "ch"), check_vma=False
    )
```

```python
import math

import jax
import jax.numpy as jnp
import numpy as np
from jax import lax
from jax.experimental import pallas as pl
from jax.experimental.pallas import tpu as pltpu
from jax.sharding import PartitionSpec as P

ROWS = 256
COLUMNS = 256
LENGTH = 65536
BF16 = jnp.bfloat16
F32 = jnp.float32
MESH = pl.DeviceIdType.MESH


PITCH = 24


def table():
    counter = np.arange(256)
    product = counter[:, None] * counter[None, :]
    angle = product % 256 * (2.0 * math.pi / 256)
    twist = product * (2.0 * math.pi / LENGTH)
    parts = [np.cos(angle), np.sin(angle), np.cos(twist), np.sin(twist)]
    return jnp.asarray(np.stack(parts), F32)


def flip(v, mask):
    if mask == 0:
        return v
    if mask == 1:
        return v + 1 - 2 * lax.rem(v, 2)
    if mask == 2:
        return lax.rem(v + 2, 4)
    return 3 - v


def dot(a, b):
    return jnp.dot(a, b, preferred_element_type=F32)


def flip2(v, step):
    return lax.rem(v + jnp.where(step == 3, 2, jnp.where(step == 2, 3, step)), 4)


def kernel(
    signal, spectrum, w_hbm, mode_hbm, gain_hbm, table_hbm,
    out,
    raw, raw2, turned, sig, spec, twist, w, mode, gain,
    first, second, third, last, scatter, regroup, order,
    buf, final, spectral, mixed, hid, send, gathered, rows, total, wmine, wfull, prod,
    h_sems, a_sems, b_sems, w_sems, d_sems, met,
):
    s = lax.axis_index("seq")
    c = lax.axis_index("ch")
    z, y, x, k = s // 4, lax.rem(s, 4), c // 2, lax.rem(c, 2)
    other = 1 - k

    def zdev(mask):
        return {"seq": flip(z, mask) * 4 + y, "ch": c}

    def ydev(mask):
        return {"seq": z * 4 + flip(y, mask), "ch": c}

    def xdev(mask):
        return {"seq": s, "ch": flip(x, mask) * 2 + k}

    partner = {"seq": s, "ch": x * 2 + other}

    def copy(a, b, ss, rs, dev):
        return pltpu.make_async_remote_copy(a, b, ss, rs, device_id=dev, device_id_type=MESH)

    def recv(ref, sem):
        copy(ref, ref, sem, sem, partner).wait_recv()

    def sent(ref, sem):
        copy(ref, ref, sem, sem, partner).wait_send()

    def peers(fn):
        for mask in (2, 1, 3, 0):
            for core in (k, other):
                if mask or core is other:
                    fn(flip(x, mask) * 2 + core)

    loads = [
        pltpu.make_async_copy(signal.at[pl.ds(2 * i, 2)], raw.at[pl.ds(2 * i, 2)], h_sems.at[i])
        for i in range(8)
    ]
    loads += [
        pltpu.make_async_copy(spectrum.at[i], raw2.at[i], h_sems.at[8 + i]) for i in range(2)
    ]
    small = ((table_hbm, twist), (w_hbm, w), (mode_hbm, mode), (gain_hbm, gain))
    for i, (a, b) in enumerate(small):
        loads.append(pltpu.make_async_copy(a, b, h_sems.at[10 + i]))
    for load in loads[:8]:
        load.start()

    barrier = pltpu.get_barrier_semaphore()

    def greet(dev):
        pl.semaphore_signal(barrier, 1, device_id=dev, device_id_type=MESH)

    for mask in (1, 2, 3):
        greet(zdev(mask))
        greet(ydev(mask))
    peers(lambda t: greet({"seq": s, "ch": t}))

    def turn(source, lo, n):
        def step(a, carry):
            value = source[a].T
            turned.at[0][pl.ds(a, 128, stride=PITCH), :] = value[:, :128]
            turned.at[1][pl.ds(a, 128, stride=PITCH), :] = value[:, 128:]
            return carry

        lax.fori_loop(lo, lo + n, step, 0, unroll=min(n, 4))

    def pack(target):
        def step(t, carry):
            for h in range(2):
                for m in range(4):
                    at = pl.ds(pl.multiple_of((t * 8 + h * 4 + m) * PITCH, 8), 16)
                    value = jnp.concatenate([turned[0, at, :], turned[1, at, :]], 1)
                    target[t // 4, lax.rem(t, 4), h, m] = value.astype(BF16)
            return carry

        lax.fori_loop(0, 16, step, 0)

    for i in range(8):
        loads[i].wait()
        if i == 0:
            for load in loads[8:]:
                load.start()
        turn(raw, 2 * i, 2)
    pack(sig)
    pl.semaphore_wait(barrier, 13)

    class Plane:
        def __init__(self, grab, buf, final, sems):
            self.grab, self.buf, self.final = grab, buf, final
            self.s1, self.s2, self.rfin, self.rbuf = sems

        def dev(self, u, leg, mask):
            return zdev(mask) if u % 2 == leg else ydev(mask)

        def F(self, u):
            for mask in (2, 1, 3):
                if u % 2 == 0:
                    row = self.grab(u, flip(z, mask), slice(None))
                else:
                    row = self.grab(u, slice(None), flip(y, mask))
                to, sem = self.buf.at[u, mask - 1], self.rbuf.at[u, mask - 1]
                copy(row, to, self.s1.at[u], sem, self.dev(u, 0, mask)).start()

        def S(self, u, m1):
            if m1:
                recv(self.buf.at[u, m1 - 1], self.rbuf.at[u, m1 - 1])
            for mask in (2, 1, 3, 0):
                other = flip(y if u % 2 == 0 else z, mask)
                if m1:
                    part = self.buf.at[u, m1 - 1, other]
                else:
                    part = self.grab(u, z, other) if u % 2 == 0 else self.grab(u, other, y)
                if u % 2 == 0:
                    slot = self.final.at[u, flip(z, m1), y]
                else:
                    slot = self.final.at[u, z, flip(y, m1)]
                if mask:
                    to = self.dev(u, 1, mask)
                    copy(part, slot, self.s2.at[u], self.rfin.at[u], to).start()
                else:
                    slot[...] = part[...]

        def done(self, u):
            recv(self.final.at[u, pl.ds(0, 3)], self.rfin.at[u])

        def drain(self, u):
            sent(self.final.at[u, pl.ds(0, 3)], self.s1.at[u])
            sent(self.final.at[u, pl.ds(0, 3)], self.s2.at[u])

    def grab_inputs(u, zi, yi):
        if u < 2:
            return sig.at[zi, yi, u]
        return spec.at[u % 2, zi, yi, u // 2 - 1]

    A = Plane(grab_inputs, buf, final, a_sems)

    def twists(ch, columns=slice(None)):
        on = mode[s * 8 + ch] == 1
        tc = jnp.where(on, twist[2, :, columns], 1.0)
        return tc, jnp.where(on, twist[3, :, columns], 0.0)

    def forward(h, lo):
        def step(m, carry):
            image = final[h, :, :, m].reshape(256, 256)
            value = dot(first[...], image)
            re, im = value[:256], value[256:]
            tc, ts = twists(4 * h + m)
            pair = jnp.concatenate([re * tc + im * ts, im * tc - re * ts], 1).astype(BF16)
            spectral[4 * h + m] = dot(pair, second[...])
            return carry

        lax.fori_loop(lo, lo + 2, step, 0, unroll=True)

    def inverse(h, e):
        columns = slice(e * 128, e * 128 + 128)

        def step(j, carry):
            parts = []
            for m in (2 * j, 2 * j + 1):
                if e == 0:
                    value = spectral[4 * h + m]
                    re, im = value[:, :256], value[:, 256:]
                    fr = final[2 + 2 * h, :, :, m].reshape(256, 256).astype(F32)
                    fi = final[3 + 2 * h, :, :, m].reshape(256, 256).astype(F32)
                    pair = jnp.concatenate([re * fr - im * fi, re * fi + im * fr], 1).astype(BF16)
                    mixed[m] = pair
                else:
                    pair = mixed[m]
                value = dot(pair, third[e])
                re, im = value[:, :128], value[:, 128:]
                tc, ts = twists(4 * h + m, columns)
                pair = jnp.concatenate([re * tc - im * ts, re * ts + im * tc], 0)
                parts.append(pair.astype(BF16))
            value = dot(last[...], jnp.concatenate(parts, 1))
            for n in range(2):
                m = 2 * j + n
                image = final[h, :, :, m, :, columns].reshape(256, 128).astype(F32)
                part = value[:, n * 128 : (n + 1) * 128] + gain[s * 8 + 4 * h + m] * image
                hid[e, m] = part.astype(BF16).reshape(4, 4, 16, 128)
            return carry

        lax.fori_loop(0, 2, step, 0, unroll=True)

    def build():
        cos, sin = twist[0], twist[1]
        first[:256], first[256:] = cos.astype(BF16), (-sin).astype(BF16)
        second[:256, :256] = second[256:, 256:] = cos.astype(BF16)
        second[:256, 256:] = (-sin).astype(BF16)
        second[256:, :256] = sin.astype(BF16)
        for e in range(2):
            part = slice(e * 128, e * 128 + 128)
            third[e, :256, :128] = third[e, 256:, 128:] = cos[:, part].astype(BF16)
            third[e, 256:, :128] = (-sin[:, part]).astype(BF16)
            third[e, :256, 128:] = sin[:, part].astype(BF16)
        last[:, :256] = (cos / LENGTH).astype(BF16)
        last[:, 256:] = (-sin / LENGTH).astype(BF16)
        i = lax.broadcasted_iota(jnp.int32, (256, 256), 0)
        j = lax.broadcasted_iota(jnp.int32, (256, 256), 1)
        m, t, at = j >> 6, (j >> 4) & 3, j & 15
        row = t * 64 + ((at >> 1) & 1) * 32 + (at >> 2) * 8 + (at & 1) * 4 + m
        scatter[...] = jnp.where(i == row, 1.0, 0.0).astype(BF16)
        column = ((i >> 2) & 1) * 128 + (i >> 7) * 64 + ((i >> 3) & 15) * 4 + (i & 3)
        regroup[...] = jnp.where(j == column, 1.0, 0.0).astype(BF16)
        i, j = i[:128, :128], j[:128, :128]
        row = ((j >> 2) & 1) * 64 + (j >> 3) * 4 + (j & 3)
        order[...] = jnp.where(i == row, 1.0, 0.0).astype(BF16)

    def place(h, e):
        for t in (0, 2):
            blocks = [hid[e, :, t + n].reshape(256, 128) for n in range(2)]
            value = dot(scatter[...], jnp.concatenate(blocks, 1)).astype(BF16)
            for n in range(2):
                part = value[:, n * 128 : (n + 1) * 128]
                send[h, e, (t + n) * 32 : (t + n + 1) * 32] = part.reshape(32, 8, 128)

    sb, rb = b_sems
    mine = c * 16 + s

    def scatter_to(core, h, e):
        source, target = send.at[h, e], gathered.at[h, e]
        sem, done = sb.at[h, e], rb.at[h, e]

        def step(i, carry):
            i = 15 - i
            zz, yy = flip2(z, lax.rem(i, 4)), flip2(y, i // 4)
            block = (zz * 4 + yy) * 8 + core * 4
            for mask in (2, 1, 3, 0):
                xx = flip(x, mask)
                to = {"seq": zz * 4 + yy, "ch": xx * 2 + core}
                one = copy(source.at[block + xx], target.at[mine], sem, done, to)
                if mask:
                    one.start()
                else:

                    @pl.when(jnp.logical_or(i > 0, k != core))
                    def _():
                        one.start()

            return carry

        lax.fori_loop(0, 16, step, 0)

    def keep(h, e):
        gathered[h, e, mine] = send[h, e, s * 8 + k * 4 + x]

    ws, wr = w_sems

    def pair(method, u, *m):
        method(u, *m)
        method(u + 1, *m)

    pair(A.F, 0)
    pair(A.S, 0, 0)
    for i in range(2):
        loads[8 + i].wait()
        turn(raw2.at[i], 0, 16)
        pack(spec.at[i])
        A.F(2 + i)
    pair(A.F, 4)
    pair(A.S, 0, 1)
    pair(A.S, 0, 3)
    pair(A.S, 2, 0)
    for load in loads[10:]:
        load.wait()
    build()
    wmine[...] = dot(order[...], w[...]).astype(BF16).reshape(2, 64, 1024)
    peers(lambda t: copy(wmine, wfull.at[:, c], ws, wr, {"seq": s, "ch": t}).start())
    wfull[:, c] = wmine[...]
    pair(A.S, 0, 2)
    pair(A.S, 4, 0)
    pair(A.S, 2, 1)
    pair(A.S, 2, 3)
    pair(A.S, 2, 2)
    pair(A.S, 4, 1)
    A.done(0)
    forward(0, 0)
    pair(A.S, 4, 3)
    A.done(1)
    peers(
        lambda t: pl.semaphore_signal(
            met, 1, device_id={"seq": s, "ch": t}, device_id_type=MESH
        )
    )
    forward(0, 2)
    pair(A.S, 4, 2)
    forward(1, 0)
    forward(1, 2)
    A.done(2)
    A.done(3)
    inverse(0, 0)
    place(0, 0)
    pl.semaphore_wait(met, 7)
    scatter_to(0, 0, 0)
    inverse(0, 1)
    place(0, 1)
    A.done(4)
    A.done(5)
    scatter_to(1, 0, 0)
    inverse(1, 0)
    place(1, 0)
    scatter_to(0, 1, 0)
    scatter_to(0, 0, 1)
    inverse(1, 1)
    place(1, 1)
    scatter_to(0, 1, 1)
    scatter_to(1, 1, 0)
    scatter_to(1, 0, 1)
    scatter_to(1, 1, 1)
    for e in range(2):
        keep(0, e)
        keep(1, e)
    recv(wfull.at[:, pl.ds(0, 7)], wr)

    ds, dr = d_sems

    def arrange(h, e):
        recv(gathered.at[h, e, pl.ds(0, 127)], rb.at[h, e])
        for i in range(4):
            value = lax.dot_general(
                gathered[h, e, 32 * i : 32 * i + 32].reshape(256, 128),
                regroup[...],
                (((0,), (0,)), ((), ())),
                preferred_element_type=F32,
            ).astype(BF16)
            rows[:128, i * 128 : (i + 1) * 128] = value[:, :128]
            rows[128:, i * 128 : (i + 1) * 128] = value[:, 128:]

    def begin(e):
        arrange(0, e)
        total[...] = dot(rows[...], wfull[0].reshape(512, 1024))

    def finish(e):
        arrange(1, e)
        for mask in (2, 1, 3, 0):
            xx = flip(x, mask)
            columns = pl.ds(pl.multiple_of(xx * 256, 256), 256)
            value = dot(rows[...], wfull[1, :, :, columns].reshape(512, 256))
            value = (total[:, columns] + value).astype(BF16)
            for core in range(2):
                part = value[:, core * 128 : (core + 1) * 128]
                prod[e, xx * 2 + core] = part.reshape(2, 128, 128)
            for core in (k, other):
                if mask or core is other:
                    to = {"seq": s, "ch": xx * 2 + core}
                    part = prod.at[e, xx * 2 + core]
                    copy(part, out.at[c, :, e], ds.at[e], dr.at[e], to).start()
        out[c, :, e] = prod[e, c]

    begin(0)
    finish(0)
    begin(1)
    finish(1)
    for e in range(2):
        recv(prod.at[e, pl.ds(0, 7)], dr.at[e])

    for u in range(6):
        A.drain(u)
    for e in range(2):
        for h in range(2):
            sent(send.at[h, e, pl.ds(0, 127)], sb.at[h, e])
        sent(prod.at[e, pl.ds(0, 7)], ds.at[e])
    sent(wfull.at[:, pl.ds(0, 7)], ws)


def per_device(signal, spectrum, channel_mode, skip_gain, out_weight):
    unit = (4, 16, 256)
    dma = pltpu.SemaphoreType.DMA
    constant = table()
    vmem = pl.BlockSpec(memory_space=pltpu.VMEM)
    hbm = pl.BlockSpec(memory_space=pltpu.HBM)
    fixed = [
        pltpu.with_memory_space_constraint(t, pltpu.HBM)
        for t in (out_weight, channel_mode, skip_gain)
    ]
    result = pl.pallas_call(
        kernel,
        out_shape=jax.ShapeDtypeStruct((8, 2, 2, 128, 128), BF16),
        in_specs=[hbm] * 6,
        out_specs=vmem,
        scratch_shapes=[
            pltpu.VMEM((16, 256, 128), F32),
            pltpu.VMEM((2, 16, 256, 128), F32),
            pltpu.VMEM((2, 129 * PITCH, 128), F32),
            pltpu.VMEM((4, 4, 2) + unit, BF16),
            pltpu.VMEM((2, 4, 4, 2) + unit, BF16),
            pltpu.VMEM((4, 256, 256), F32),
            pltpu.VMEM((128, 1024), BF16),
            pltpu.SMEM((128,), jnp.int32),
            pltpu.SMEM((128,), F32),
            pltpu.VMEM((512, 256), BF16),
            pltpu.VMEM((512, 512), BF16),
            pltpu.VMEM((2, 512, 256), BF16),
            pltpu.VMEM((256, 512), BF16),
            pltpu.VMEM((256, 256), BF16),
            pltpu.VMEM((256, 256), BF16),
            pltpu.VMEM((128, 128), BF16),
            pltpu.VMEM((6, 3, 4) + unit, BF16),
            pltpu.VMEM((6, 4, 4) + unit, BF16),
            pltpu.VMEM((8, 256, 512), F32),
            pltpu.VMEM((4, 256, 512), BF16),
            pltpu.VMEM((2, 4, 4, 4, 16, 128), BF16),
            pltpu.VMEM((2, 2, 128, 8, 128), BF16),
            pltpu.VMEM((2, 2, 128, 8, 128), BF16),
            pltpu.VMEM((256, 512), BF16),
            pltpu.VMEM((256, 1024), F32),
            pltpu.VMEM((2, 64, 1024), BF16),
            pltpu.VMEM((2, 8, 64, 1024), BF16),
            pltpu.VMEM((2, 8, 2, 128, 128), BF16),
            dma((14,)),
            (dma((6,)), dma((6,)), dma((6,)), dma((6, 3))),
            (dma((2, 2)), dma((2, 2))),
            (dma, dma),
            (dma((2,)), dma((2,))),
            pltpu.SemaphoreType.REGULAR,
        ],
        compiler_params=pltpu.CompilerParams(
            collective_id=0, has_side_effects=True, vmem_limit_bytes=52 << 20
        ),
        name="hyena",
    )(
        signal.reshape(16, 256, 128), spectrum, *fixed, constant
    )
    return result.astype(F32).reshape(1, 4096, 128)


def solution(mesh):
    in_specs = (
        P(None, "seq", "ch"), P(None, "seq", None, "ch"), P("ch"), P("ch"), P("ch", None)
    )
    return jax.shard_map(
        per_device, mesh=mesh, in_specs=in_specs, out_specs=P(None, "seq", "ch"), check_vma=False
    )
```
